32 devices in a mesh: tp: 4 (over z), dp: 8 (over y, x, core).
Axes of the slice: x: 2, y: 2, z: 4, core: 2. Of those that a mesh axis runs over, the one named last changes fastest.
Arguments:
- a_mat: bfloat16 [5120, 32768], P(('dp', 'tp'))
- b_mat: bfloat16 [32768, 13824], P(('dp', 'tp'))
Outputs:
- output: bfloat16 [5120, 13824], P(('dp', 'tp'))
All inputs are finite; a program needn't handle non-finite values.
Results may differ from the reference program's by a relative error of at most 0.001.
Values are sent between devices in bfloat16 or wider.
A program may use at most 1 GiB of HBM per device.

```python
import jax
import jax.numpy as jnp

D_MODEL = 5120
D_FF = 13824
TOKENS_DEV = 1024
DEVICES = 32
TOKENS = TOKENS_DEV * DEVICES


def setup_inputs(seed: int = 0) -> dict:
    root_key = jax.random.key(seed)
    key_a, key_b = jax.random.split(root_key)
    acts_t = jax.random.normal(key_a, (D_MODEL, TOKENS), jnp.float32)
    grads = jax.random.normal(key_b, (TOKENS, D_FF), jnp.float32) * (TOKENS ** -0.5)
    return {"a_mat": acts_t.astype(jnp.bfloat16), "b_mat": grads.astype(jnp.bfloat16)}


def reference(a_mat, b_mat):
    prod = jnp.dot(a_mat, b_mat, preferred_element_type=jnp.float32)
    return prod.astype(jnp.bfloat16)
```

```python
import functools

import jax
import jax.numpy as jnp
from jax import lax
from jax.experimental import pallas as pl
from jax.experimental.pallas import tpu as pltpu
from jax.sharding import PartitionSpec as P

TILE = 384
LAG = 6
B_SEND, B_PASS, B_HAVE, A_SEND, A_PASS, A_HAVE, MULT, SUM = range(8)

ROW_ORDER = ((1, 2, 3, 0), (2, 3, 0, 1), (1, 0, 3, 2), (2, 1, 0, 3))
A_DEST = ((1, 3, 2), (0, 3, 2), (3, 0, 1), (2, 0, 1))


def make_steps(tiles):
    arrivals = ["B", "B", "A", "B", "A", "B", "B", "A"] + ["B"] * (tiles - 5) + ["A"]
    seq = [(what, arrivals[:n].count(what)) for n, what in enumerate(arrivals)]
    steps, sums = [], []
    have_a, have_b = [], []
    last = [None, None]

    def comm(op_b, op_a, item):
        steps.append((op_b, 0, item[1], 0, 0) if item[0] == "B" else (op_a, item[1], 0, 0, 0))

    def mult(u, j):
        steps.append((MULT, u, j, int(last[0] != u), int(last[1] != j)))
        last[0], last[1] = u, j

    done = 0
    comm(B_SEND, A_SEND, seq[0])
    for n, item in enumerate(seq):
        comm(B_PASS, A_PASS, item)
        if n + 1 < len(seq):
            comm(B_SEND, A_SEND, seq[n + 1])
        comm(B_HAVE, A_HAVE, item)
        if item[0] == "B":
            have_b.append(item[1])
            for u in (2, 1, 0):
                if u in have_a:
                    mult(u, item[1])
            sums += [(u, item[1]) for u in (1, 0, 2) if u in have_a]
        else:
            have_a.append(item[1])
            for j in have_b:
                mult(item[1], j)
            sums += [(item[1], j) for j in have_b]
        while done < len(sums) - LAG and sums[done][0] < 3:
            steps.append((SUM, *sums[done], 0, 0))
            done += 1
    rest = [s for s in sums[done:] if s[0] < 3]
    for j in range(tiles):
        now = [s for s in rest if s[1] == j]
        steps += [(SUM, *s, 0, 0) for s in [*now, (3, j)]]
    return steps


def choose(index, values):
    out = jnp.int32(values[-1])
    for k in range(len(values) - 2, -1, -1):
        if values[k] != values[k + 1] or k == 0:
            out = jnp.where(index <= k, jnp.int32(values[k]), out)
    return out


def kernel(
    steps, a, b, c_out, a_all, b_all, part, low, high,
    av, bv, acc, s0, s1, s2, cv,
    a1_s, a1_r, ax_s, ax_r, ay_s, ay_r, fx_s, fx_r, fy_s, fy_r,
    b_s, b_r, own_s, own_r, pass_s, pass_r, up_s, low_r, high_r, fin_s, fin_r, fin_l, lda, ldb, st, ls,
):
    rows, depth = a.shape[0], b.shape[0]
    tile = part.shape[3]
    tiles = part.shape[1]
    wide = tile * tiles
    half = rows // 2
    z, d = lax.axis_index("tp"), lax.axis_index("dp")
    q = d // 2
    core, x, y = d % 2, q % 2, d // 4
    q_x, q_y = q + 1 - 2 * x, q + 2 - 4 * y
    q_d = q_x + 2 - 4 * y
    peers = (q_x, q_y, q_d)

    def at(plane, chip):
        return {"tp": plane, "dp": chip * 2 + core}

    sibling = {"tp": z, "dp": d + 1 - 2 * core}

    def remote(src, dst, send, recv, to):
        return pltpu.make_async_remote_copy(
            src_ref=src, dst_ref=dst, send_sem=send, recv_sem=recv, device_id=to, device_id_type=pl.DeviceIdType.MESH
        )

    def row_group(u):
        return choose(z * 4 + u, [i for order in ROW_ORDER for i in order])

    def a_rows(i, chip, first=0, count=rows):
        return a_all.at[i, pl.ds(pl.multiple_of(chip * rows + first, half), count), :]

    def b_rows(j, dev):
        return b_all.at[j, pl.ds(pl.multiple_of(dev * depth, depth), depth), :]

    def columns(chip, j):
        return pl.ds(pl.multiple_of(chip * wide + j * tile, tile), tile)

    def k_block(dev, plane):
        return pl.ds(pl.multiple_of((dev * 4 + plane) * depth, depth), depth)

    barrier = pltpu.get_barrier_semaphore()
    for plane in range(1, 4):
        pl.semaphore_signal(barrier, inc=1, device_id=at((z + plane) % 4, q), device_id_type=pl.DeviceIdType.MESH)
    for chip in peers:
        pl.semaphore_signal(barrier, inc=1, device_id=at(z, chip), device_id_type=pl.DeviceIdType.MESH)
    pl.semaphore_signal(barrier, inc=1, device_id=sibling, device_id_type=pl.DeviceIdType.MESH)
    pl.semaphore_wait(barrier, 7)

    def a1(m, dev):
        plane = choose(z * 3 + m, [p for dest in A_DEST for p in dest])
        return remote(
            a.at[:, k_block(dev, plane)],
            a_all.at[z, pl.ds(pl.multiple_of(q * rows, half), rows), pl.ds(pl.multiple_of(dev * depth, depth), depth)],
            a1_s.at[m], a1_r.at[z], at(plane, q),
        )

    for m in range(3):

        @pl.loop(0, 8)
        def _(dev):
            a1(m, dev).start()

    own_in = [pltpu.make_async_copy(a.at[:, k_block(dev, z)], av.at[dev, pl.ds(0, rows), :], lda.at[dev]) for dev in range(8)]
    own_out = [
        pltpu.make_async_copy(
            av.at[dev, pl.ds(0, rows), :],
            a_all.at[z, pl.ds(pl.multiple_of(q * rows, half), rows), pl.ds(dev * depth, depth)],
            ldb.at[dev],
        )
        for dev in range(8)
    ]
    for copy in own_in:
        copy.start()
    for copy, put in zip(own_in, own_out, strict=True):
        copy.wait()
        put.start()
    for put in own_out:
        put.wait()

    def b_copy(j, n):
        return remote(b.at[:, columns(peers[n], j)], b_rows(j, d), b_s.at[j, n], b_r.at[j, n], at(z, peers[n]))

    def b_landed(j, n):
        dst = b_rows(j, peers[n] * 2 + core)
        return remote(dst, dst, b_s.at[j, n], b_r.at[j, n], at(z, peers[n]))

    def b_own(j):
        return remote(b.at[:, columns(q, j)], b_rows(j, d), own_s.at[j], own_r.at[j], sibling)

    def b_pass(j, n):
        dst = b_rows(j, peers[n] * 2 + core)
        return remote(dst, dst, pass_s.at[j, n], pass_r.at[j, n], sibling)

    def b_passed(j, n):
        dst = b_rows(j, peers[n] * 2 + 1 - core)
        return remote(dst, dst, pass_s.at[j, n], pass_r.at[j, n], sibling)

    def b_own_passed(j):
        dst = b_rows(j, d + 1 - 2 * core)
        return remote(dst, dst, own_s.at[j], own_r.at[j], sibling)

    def a_x(u, i, chip):
        return remote(a_rows(i, chip), a_rows(i, chip), ax_s.at[u], ax_r.at[u], at(z, q_x))

    def a_y(u, i, chip):
        return remote(a_rows(i, chip), a_rows(i, chip), ay_s.at[u], ay_r.at[u], at(z, q_y))

    def f_y(u, i, chip):
        return remote(a_rows(i, chip, 0, half), a_rows(i, chip, 0, half), fy_s.at[u], fy_r.at[u], at(z, q_y))

    def f_x(u, i, chip):
        return remote(a_rows(i, chip, half, half), a_rows(i, chip, half, half), fx_s.at[u], fx_r.at[u], at(z, q_x))

    def up(i, j):
        return remote(part.at[i, j], low.at[i, j], up_s.at[i, j], low_r.at[i, j], at(jnp.minimum(z + 1, 3), q))

    def down(i, j):
        return remote(part.at[i, j], high.at[i, j], up_s.at[i, j], high_r.at[i, j], at(jnp.maximum(z - 1, 0), q))

    def send_part(i, j):
        @pl.when(i > z)
        def _():
            up(i, j).start()

        @pl.when(i < z)
        def _():
            down(i, j).start()

    def final(j, n):
        return remote(
            cv.at[j % 2, pl.ds(pl.multiple_of(peers[n] * rows, half), rows), :],
            c_out.at[:, columns(q, j)],
            fin_s.at[j, n], fin_r.at[j, n], at(z, peers[n]),
        )

    def final_landed(j, n):
        dst = c_out.at[:, columns(peers[n], j)]
        return remote(cv.at[j % 2, pl.ds(0, rows), :], dst, fin_s.at[j, n], fin_r.at[j, n], at(z, peers[n]))

    def final_own(j):
        return pltpu.make_async_copy(
            cv.at[j % 2, pl.ds(pl.multiple_of(q * rows, half), rows), :], c_out.at[:, columns(q, j)], fin_l.at[j % 2]
        )

    def load_a(i, k):
        dev = (d + k) % 8
        return pltpu.make_async_copy(a_all.at[i, :, pl.ds(pl.multiple_of(dev * depth, depth), depth)], av.at[k], lda.at[k])

    def load_b(j, k):
        return pltpu.make_async_copy(b_rows(j, (d + k) % 8), bv.at[k], ldb.at[k])

    def load_b_own(j):
        return pltpu.make_async_copy(b.at[:, columns(q, j)], bv.at[0], ldb.at[0])

    def multiply(u, j, new_a, new_b):
        i = row_group(u)

        @pl.when(new_b == 1)
        def _():
            load_b_own(j).start()

        @pl.when(new_a == 1)
        def _():
            load_a(i, 0).start()

        @pl.loop(1, 8)
        def _(k):
            @pl.when(new_b == 1)
            def _():
                load_b(j, k).start()

            @pl.when(new_a == 1)
            def _():
                load_a(i, k).start()

        acc[...] = jnp.zeros_like(acc)

        @pl.loop(0, 8)
        def _(k):
            @pl.when(new_a == 1)
            def _():
                load_a(i, k).wait()

            @pl.when(new_b == 1)
            def _():
                load_b(j, k).wait()

            acc[...] += jnp.dot(av[k], bv[k], preferred_element_type=jnp.float32)

        put = pltpu.make_async_copy(acc, part.at[i, j], st)
        put.start()
        put.wait()

        @pl.when(((z == 0) | (z == 3)) & (i != z))
        def _():
            send_part(i, j)

    def add_up(u, j):
        i = row_group(u)
        has_low = (z > 0) & (z <= i)
        has_high = (z < 3) & (z >= i)

        @pl.when((z == 1) | (z == 2) | (u == 3))
        def _():
            mine = pltpu.make_async_copy(part.at[i, j], s0, ls.at[0])
            below = pltpu.make_async_copy(low.at[i, j], s1, ls.at[1])
            above = pltpu.make_async_copy(high.at[i, j], s2, ls.at[2])
            mine.start()

            @pl.when(has_low)
            def _():
                up(i, j).wait_recv()
                below.start()

            @pl.when(has_high)
            def _():
                down(i, j).wait_recv()
                above.start()

            mine.wait()

            @pl.when(has_low)
            def _():
                below.wait()
                s0[...] += s1[...]

            @pl.when(has_high)
            def _():
                above.wait()
                s0[...] += s2[...]

            @pl.when(i == z)
            def _():
                @pl.when(j >= 2)
                def _():
                    for n in range(3):
                        final(j - 2, n).wait_send()
                    final_own(j - 2).wait()

                cv[j % 2] = s0[...].astype(cv.dtype)
                for n in range(3):
                    final(j, n).start()
                final_own(j).start()

            @pl.when(i != z)
            def _():
                put = pltpu.make_async_copy(s0, part.at[i, j], st)
                put.start()
                put.wait()
                send_part(i, j)

    codes = [op | u << 3 | j << 5 | new_a << 10 | new_b << 11 for op, u, j, new_a, new_b in steps]

    @pl.loop(0, len(steps))
    def _(t):
        code = choose(t, codes)
        op, u, j, new_a, new_b = code % 8, code // 8 % 4, code // 32 % 32, code // 1024 % 2, code // 2048
        i = row_group(u)

        @pl.when(op == B_SEND)
        def _():
            for n in range(3):
                b_copy(j, n).start()
            b_own(j).start()

        @pl.when(op == B_PASS)
        def _():
            for n in range(3):
                b_landed(j, n).wait_recv()
                b_pass(j, n).start()

        @pl.when(op == B_HAVE)
        def _():
            b_own_passed(j).wait_recv()
            for n in range(3):
                b_passed(j, n).wait_recv()

        @pl.when(op == A_SEND)
        def _():
            @pl.when(i != z)
            def _():
                landed = a_rows(i, q)
                remote(landed, landed, a1_s.at[0], a1_r.at[i], at(z, q_x)).wait_recv()

            a_x(u, i, q).start()
            a_y(u, i, q).start()

        @pl.when(op == A_PASS)
        def _():
            a_x(u, i, q_x).wait_recv()
            f_y(u, i, q_x).start()
            a_y(u, i, q_y).wait_recv()
            f_x(u, i, q_y).start()

        @pl.when(op == A_HAVE)
        def _():
            f_y(u, i, q_d).wait_recv()
            f_x(u, i, q_d).wait_recv()

        @pl.when(op == MULT)
        def _():
            multiply(u, j, new_a, new_b)

        @pl.when(op == SUM)
        def _():
            add_up(u, j)

    for m in range(3):
        remote(a_rows(z, q), a_rows(z, q), a1_s.at[m], a1_r.at[z], at(z, q_x)).wait_send()

    @pl.loop(0, 4)
    def _(u):
        i = row_group(u)
        a_x(u, i, q).wait_send()
        a_y(u, i, q).wait_send()
        f_y(u, i, q_x).wait_send()
        f_x(u, i, q_y).wait_send()

    @pl.loop(0, tiles)
    def _(j):
        for n in range(3):
            b_copy(j, n).wait_send()
            b_pass(j, n).wait_send()
        b_own(j).wait_send()

        @pl.loop(0, 3)
        def _(u):
            up(row_group(u), j).wait_send()

        for n in range(3):
            final_landed(j, n).wait_recv()

    @pl.loop(tiles - 2, tiles)
    def _(j):
        for n in range(3):
            final(j, n).wait_send()
        final_own(j).wait()


def solution(mesh):
    spec_rows = P(("dp", "tp"), None)

    def local_block(a, b):
        rows, depth, cols = a.shape[0], b.shape[0], b.shape[1]
        wide = cols // 4
        tile = min(TILE, wide // 9)
        tiles = wide // tile
        group = 4 * rows
        steps = make_steps(tiles)
        dma = pltpu.SemaphoreType.DMA
        any_space = pl.BlockSpec(memory_space=pl.ANY)
        out = pl.pallas_call(
            functools.partial(kernel, steps),
            out_shape=[
                jax.ShapeDtypeStruct((rows, cols), jnp.bfloat16),
                jax.ShapeDtypeStruct((4, group, 8 * depth), jnp.bfloat16),
                jax.ShapeDtypeStruct((tiles, 8 * depth, tile), jnp.bfloat16),
                jax.ShapeDtypeStruct((4, tiles, group, tile), jnp.float32),
                jax.ShapeDtypeStruct((4, tiles, group, tile), jnp.float32),
                jax.ShapeDtypeStruct((4, tiles, group, tile), jnp.float32),
            ],
            in_specs=[any_space] * 2,
            out_specs=[any_space] * 6,
            scratch_shapes=[
                pltpu.VMEM((8, group, depth), jnp.bfloat16),
                pltpu.VMEM((8, depth, tile), jnp.bfloat16),
                pltpu.VMEM((group, tile), jnp.float32),
                pltpu.VMEM((group, tile), jnp.float32),
                pltpu.VMEM((group, tile), jnp.float32),
                pltpu.VMEM((group, tile), jnp.float32),
                pltpu.VMEM((2, group, tile), jnp.bfloat16),
                dma((3,)), dma((4,)),
                dma((4,)), dma((4,)), dma((4,)), dma((4,)),
                dma((4,)), dma((4,)), dma((4,)), dma((4,)),
                dma((tiles, 3)), dma((tiles, 3)), dma((tiles,)), dma((tiles,)), dma((tiles, 3)), dma((tiles, 3)),
                dma((4, tiles)), dma((4, tiles)), dma((4, tiles)),
                dma((tiles, 3)), dma((tiles, 3)), dma((2,)),
                dma((8,)), dma((8,)), dma, dma((3,)),
            ],
            compiler_params=pltpu.CompilerParams(
                collective_id=0, has_side_effects=True, vmem_limit_bytes=60 * 1024 * 1024
            ),
        )(a, b)
        return out[0]

    return jax.shard_map(local_block, mesh=mesh, in_specs=(spec_rows, spec_rows), out_specs=spec_rows, check_vma=False)
```

```python
import functools

import jax
import jax.numpy as jnp
from jax import lax
from jax.experimental import pallas as pl
from jax.experimental.pallas import tpu as pltpu
from jax.sharding import PartitionSpec as P

TILE = 384
B_SEND, B_PASS, B_HAVE, A_SEND, A_PASS, A_HAVE, MULT, SUM, A_OUT, NOTHING = range(10)
LETTERS = "bphafgmso"

END_ORDER = (
    "b05b02b06o10a20p05p02o20h05b01o30p01f20b08p06g20m25a30h02m22",
    "h01p08h08m21h06m28f30b04m26b03g30m35b00m36m31p04h04m38p03m24",
    "m34h03m33a10p00b07h00m32m30m23p07f10h07a00m37m20g10m15m18m14",
    "m12f00m27m13m16g00m04m00m01s01m08m05s04s00m02s02s08s05m11m17",
    "m07s07m10m03m06s06s03",
)
MID_ORDER = (
    "o30b03b06b02o20b01b08o00p02b04p01b05p05a30p04p03p06h06a20h04",
    "f30h05p08f20h03b07g30m35m36m34s36h02g20s35m25m24s25a00m26h01",
    "m31h08s31s26m28p07m23s28m21b00m32h07s34m37m38m27f00s32m33p00",
    "a10s38m22h00m30s21s24g00s30s22m04s04m05m08m02s05m00f10m07s02",
    "m01m20s01s37g10m14s00s23s33s14m18s20s18s08m03m17s07m16m12s12",
    "m15s03s27s16m06s15s06m11m13s13s17s11m10s10",
)


def make_steps(order):
    steps = []
    last_i, last_j = -1, -1
    order = "".join(order)
    for n in range(0, len(order), 3):
        op, i, j = LETTERS.index(order[n]), int(order[n + 1]), int(order[n + 2])
        new = (0, 0)
        if op == MULT:
            new = (int(last_i != i), int(last_j != j))
            last_i, last_j = i, j
        steps.append((op, i, j, *new))
    return steps


def choose(index, values):
    out = jnp.int32(values[-1])
    for k in range(len(values) - 2, -1, -1):
        if values[k] != values[k + 1] or k == 0:
            out = jnp.where(index <= k, jnp.int32(values[k]), out)
    return out


def kernel(
    end_steps, mid_steps, a, b, c_out, a_all, b_all, part, low, high,
    av, bv, acc, s0, s1, s2, cv,
    a1_s, a1_r, ax_s, ax_r, ay_s, ay_r, fx_s, fx_r, fy_s, fy_r,
    b_s, b_r, own_s, own_r, pass_s, pass_r, up_s, low_r, high_r, fin_s, fin_r, fin_l, lda, ldb, st, ls,
):
    rows, depth = a.shape[0], b.shape[0]
    tile = part.shape[3]
    tiles = part.shape[1]
    wide = tile * tiles
    half = rows // 2
    z, d = lax.axis_index("tp"), lax.axis_index("dp")
    q = d // 2
    core, x, y = d % 2, q % 2, d // 4
    q_x, q_y = q + 1 - 2 * x, q + 2 - 4 * y
    q_d = q_x + 2 - 4 * y
    peers = (q_x, q_y, q_d)

    def at(plane, chip):
        return {"tp": plane, "dp": chip * 2 + core}

    sibling = {"tp": z, "dp": d + 1 - 2 * core}

    def remote(src, dst, send, recv, to):
        return pltpu.make_async_remote_copy(
            src_ref=src, dst_ref=dst, send_sem=send, recv_sem=recv, device_id=to, device_id_type=pl.DeviceIdType.MESH
        )

    def a_rows(i, chip, first=0, count=rows):
        return a_all.at[i, pl.ds(pl.multiple_of(chip * rows + first, half), count), :]

    def b_rows(j, dev):
        return b_all.at[j, pl.ds(pl.multiple_of(dev * depth, depth), depth), :]

    def columns(chip, j):
        return pl.ds(pl.multiple_of(chip * wide + j * tile, tile), tile)

    def k_block(dev, plane):
        return pl.ds(pl.multiple_of((dev * 4 + plane) * depth, depth), depth)

    barrier = pltpu.get_barrier_semaphore()
    for plane in range(1, 4):
        pl.semaphore_signal(barrier, inc=1, device_id=at((z + plane) % 4, q), device_id_type=pl.DeviceIdType.MESH)
    for chip in peers:
        pl.semaphore_signal(barrier, inc=1, device_id=at(z, chip), device_id_type=pl.DeviceIdType.MESH)
    pl.semaphore_signal(barrier, inc=1, device_id=sibling, device_id_type=pl.DeviceIdType.MESH)
    pl.semaphore_wait(barrier, 7)

    def a_out(plane, dev):
        return remote(
            a.at[:, k_block(dev, plane)],
            a_all.at[z, pl.ds(pl.multiple_of(q * rows, half), rows), pl.ds(pl.multiple_of(dev * depth, depth), depth)],
            a1_s.at[plane], a1_r.at[z], at(plane, q),
        )

    own_in = [pltpu.make_async_copy(a.at[:, k_block(dev, z)], av.at[dev, pl.ds(0, rows), :], lda.at[dev]) for dev in range(8)]
    own_out = [
        pltpu.make_async_copy(
            av.at[dev, pl.ds(0, rows), :],
            a_all.at[z, pl.ds(pl.multiple_of(q * rows, half), rows), pl.ds(dev * depth, depth)],
            ldb.at[dev],
        )
        for dev in range(8)
    ]
    for copy in own_in:
        copy.start()
    for copy, put in zip(own_in, own_out, strict=True):
        copy.wait()
        put.start()
    for put in own_out:
        put.wait()

    def b_copy(j, n):
        return remote(b.at[:, columns(peers[n], j)], b_rows(j, d), b_s.at[j, n], b_r.at[j, n], at(z, peers[n]))

    def b_landed(j, n):
        dst = b_rows(j, peers[n] * 2 + core)
        return remote(dst, dst, b_s.at[j, n], b_r.at[j, n], at(z, peers[n]))

    def b_own(j):
        return remote(b.at[:, columns(q, j)], b_rows(j, d), own_s.at[j], own_r.at[j], sibling)

    def b_pass(j, n):
        dst = b_rows(j, peers[n] * 2 + core)
        return remote(dst, dst, pass_s.at[j, n], pass_r.at[j, n], sibling)

    def b_passed(j, n):
        dst = b_rows(j, peers[n] * 2 + 1 - core)
        return remote(dst, dst, pass_s.at[j, n], pass_r.at[j, n], sibling)

    def b_own_passed(j):
        dst = b_rows(j, d + 1 - 2 * core)
        return remote(dst, dst, own_s.at[j], own_r.at[j], sibling)

    def a_x(i, chip):
        return remote(a_rows(i, chip), a_rows(i, chip), ax_s.at[i], ax_r.at[i], at(z, q_x))

    def a_y(i, chip):
        return remote(a_rows(i, chip), a_rows(i, chip), ay_s.at[i], ay_r.at[i], at(z, q_y))

    def f_y(i, chip):
        return remote(a_rows(i, chip, 0, half), a_rows(i, chip, 0, half), fy_s.at[i], fy_r.at[i], at(z, q_y))

    def f_x(i, chip):
        return remote(a_rows(i, chip, half, half), a_rows(i, chip, half, half), fx_s.at[i], fx_r.at[i], at(z, q_x))

    def up(i, j):
        return remote(part.at[i, j], low.at[i, j], up_s.at[i, j], low_r.at[i, j], at(jnp.minimum(z + 1, 3), q))

    def down(i, j):
        return remote(part.at[i, j], high.at[i, j], up_s.at[i, j], high_r.at[i, j], at(jnp.maximum(z - 1, 0), q))

    def send_part(i, j):
        @pl.when(i > z)
        def _():
            up(i, j).start()

        @pl.when(i < z)
        def _():
            down(i, j).start()

    def final(j, n):
        return remote(
            cv.at[j, pl.ds(pl.multiple_of(peers[n] * rows, half), rows), :],
            c_out.at[:, columns(q, j)],
            fin_s.at[j, n], fin_r.at[j, n], at(z, peers[n]),
        )

    def final_landed(j, n):
        dst = c_out.at[:, columns(peers[n], j)]
        return remote(cv.at[j, pl.ds(0, rows), :], dst, fin_s.at[j, n], fin_r.at[j, n], at(z, peers[n]))

    def final_own(j):
        return pltpu.make_async_copy(
            cv.at[j, pl.ds(pl.multiple_of(q * rows, half), rows), :], c_out.at[:, columns(q, j)], fin_l.at[j]
        )

    def load_a(i, k):
        dev = (d + k) % 8
        return pltpu.make_async_copy(a_all.at[i, :, pl.ds(pl.multiple_of(dev * depth, depth), depth)], av.at[k], lda.at[k])

    def load_b(j, k):
        return pltpu.make_async_copy(b_rows(j, (d + k) % 8), bv.at[k], ldb.at[k])

    def load_b_own(j):
        return pltpu.make_async_copy(b.at[:, columns(q, j)], bv.at[0], ldb.at[0])

    def multiply(i, j, new_a, new_b):
        @pl.when(new_b == 1)
        def _():
            load_b_own(j).start()

        @pl.when(new_a == 1)
        def _():
            load_a(i, 0).start()

        @pl.loop(1, 8)
        def _(k):
            @pl.when(new_b == 1)
            def _():
                load_b(j, k).start()

            @pl.when(new_a == 1)
            def _():
                load_a(i, k).start()

        acc[...] = jnp.zeros_like(acc)

        @pl.loop(0, 8)
        def _(k):
            @pl.when(new_a == 1)
            def _():
                load_a(i, k).wait()

            @pl.when(new_b == 1)
            def _():
                load_b(j, k).wait()

            acc[...] += jnp.dot(av[k], bv[k], preferred_element_type=jnp.float32)

        put = pltpu.make_async_copy(acc, part.at[i, j], st)
        put.start()
        put.wait()

        @pl.when(((z == 0) | (z == 3)) & (i != z))
        def _():
            send_part(i, j)

    def add_up(i, j):
        has_low = (z > 0) & (z <= i)
        has_high = (z < 3) & (z >= i)

        if True:
            mine = pltpu.make_async_copy(part.at[i, j], s0, ls.at[0])
            below = pltpu.make_async_copy(low.at[i, j], s1, ls.at[1])
            above = pltpu.make_async_copy(high.at[i, j], s2, ls.at[2])
            mine.start()

            @pl.when(has_low)
            def _():
                up(i, j).wait_recv()
                below.start()

            @pl.when(has_high)
            def _():
                down(i, j).wait_recv()
                above.start()

            mine.wait()

            @pl.when(has_low)
            def _():
                below.wait()
                s0[...] += s1[...]

            @pl.when(has_high)
            def _():
                above.wait()
                s0[...] += s2[...]

            @pl.when(i == z)
            def _():
                cv[j] = s0[...].astype(cv.dtype)
                for n in range(3):
                    final(j, n).start()
                final_own(j).start()

            @pl.when(i != z)
            def _():
                put = pltpu.make_async_copy(s0, part.at[i, j], st)
                put.start()
                put.wait()
                send_part(i, j)

    def codes(order):
        return [op | i << 4 | j << 6 | new_a << 10 | new_b << 11 for op, i, j, new_a, new_b in order]

    end_codes, mid_codes = codes(end_steps), codes(mid_steps)
    count = max(len(end_codes), len(mid_codes))
    end_codes += [NOTHING] * (count - len(end_codes))
    mid_codes += [NOTHING] * (count - len(mid_codes))
    is_end = (z == 0) | (z == 3)

    @pl.loop(0, count)
    def _(t):
        code = jnp.where(is_end, choose(t, end_codes), choose(t, mid_codes))
        op, j, new_a, new_b = code % 16, code // 64 % 16, code // 1024 % 2, code // 2048
        i = code // 16 % 4
        i = jnp.where(z >= 2, 3 - i, i)

        @pl.when(op == B_SEND)
        @jax.named_scope("b_send")
        def _():
            for n in range(3):
                b_copy(j, n).start()
            b_own(j).start()

        @pl.when(op == B_PASS)
        @jax.named_scope("b_pass")
        def _():
            for n in range(3):
                b_landed(j, n).wait_recv()
                b_pass(j, n).start()

        @pl.when(op == B_HAVE)
        @jax.named_scope("b_have")
        def _():
            b_own_passed(j).wait_recv()
            for n in range(3):
                b_passed(j, n).wait_recv()

        @pl.when(op == A_SEND)
        @jax.named_scope("a_send")
        def _():
            @pl.when(i != z)
            def _():
                landed = a_rows(i, q)
                remote(landed, landed, a1_s.at[0], a1_r.at[i], at(z, q_x)).wait_recv()

            a_x(i, q).start()
            a_y(i, q).start()

        @pl.when(op == A_PASS)
        @jax.named_scope("a_pass")
        def _():
            a_x(i, q_x).wait_recv()
            f_y(i, q_x).start()
            a_y(i, q_y).wait_recv()
            f_x(i, q_y).start()

        @pl.when(op == A_HAVE)
        @jax.named_scope("a_have")
        def _():
            f_y(i, q_d).wait_recv()
            f_x(i, q_d).wait_recv()

        @pl.when(op == A_OUT)
        def _():
            @pl.loop(0, 8)
            def _(dev):
                a_out(i, dev).start()

        @pl.when(op == MULT)
        @jax.named_scope("mult")
        def _():
            multiply(i, j, new_a, new_b)

        @pl.when(op == SUM)
        @jax.named_scope("sum")
        def _():
            add_up(i, j)

    @pl.loop(0, 4)
    def _(i):
        @pl.when(i != z)
        def _():
            remote(a_rows(z, q), a_rows(z, q), a1_s.at[i], a1_r.at[z], at(z, q_x)).wait_send()

        a_x(i, q).wait_send()
        a_y(i, q).wait_send()
        f_y(i, q_x).wait_send()
        f_x(i, q_y).wait_send()

    @pl.loop(0, tiles)
    def _(j):
        for n in range(3):
            b_copy(j, n).wait_send()
            b_pass(j, n).wait_send()
        b_own(j).wait_send()

        @pl.loop(0, 4)
        def _(i):
            @pl.when(i != z)
            def _():
                up(i, j).wait_send()

        for n in range(3):
            final_landed(j, n).wait_recv()
            final(j, n).wait_send()
        final_own(j).wait()


def solution(mesh):
    spec_rows = P(("dp", "tp"), None)

    def local_block(a, b):
        rows, depth, cols = a.shape[0], b.shape[0], b.shape[1]
        wide = cols // 4
        tile = min(TILE, wide // 9)
        tiles = wide // tile
        group = 4 * rows
        dma = pltpu.SemaphoreType.DMA
        any_space = pl.BlockSpec(memory_space=pl.ANY)
        out = pl.pallas_call(
            functools.partial(kernel, make_steps(END_ORDER), make_steps(MID_ORDER)),
            out_shape=[
                jax.ShapeDtypeStruct((rows, cols), jnp.bfloat16),
                jax.ShapeDtypeStruct((4, group, 8 * depth), jnp.bfloat16),
                jax.ShapeDtypeStruct((tiles, 8 * depth, tile), jnp.bfloat16),
                jax.ShapeDtypeStruct((4, tiles, group, tile), jnp.float32),
                jax.ShapeDtypeStruct((4, tiles, group, tile), jnp.float32),
                jax.ShapeDtypeStruct((4, tiles, group, tile), jnp.float32),
            ],
            in_specs=[any_space] * 2,
            out_specs=[any_space] * 6,
            scratch_shapes=[
                pltpu.VMEM((8, group, depth), jnp.bfloat16),
                pltpu.VMEM((8, depth, tile), jnp.bfloat16),
                pltpu.VMEM((group, tile), jnp.float32),
                pltpu.VMEM((group, tile), jnp.float32),
                pltpu.VMEM((group, tile), jnp.float32),
                pltpu.VMEM((group, tile), jnp.float32),
                pltpu.VMEM((tiles, group, tile), jnp.bfloat16),
                dma((4,)), dma((4,)),
                dma((4,)), dma((4,)), dma((4,)), dma((4,)),
                dma((4,)), dma((4,)), dma((4,)), dma((4,)),
                dma((tiles, 3)), dma((tiles, 3)), dma((tiles,)), dma((tiles,)), dma((tiles, 3)), dma((tiles, 3)),
                dma((4, tiles)), dma((4, tiles)), dma((4, tiles)),
                dma((tiles, 3)), dma((tiles, 3)), dma((tiles,)),
                dma((8,)), dma((8,)), dma, dma((3,)),
            ],
            compiler_params=pltpu.CompilerParams(
                collective_id=0, has_side_effects=True, vmem_limit_bytes=60 * 1024 * 1024
            ),
        )(a, b)
        return out[0]

    return jax.shard_map(local_block, mesh=mesh, in_specs=(spec_rows, spec_rows), out_specs=spec_rows, check_vma=False)
```

```python
import functools

import jax
import jax.numpy as jnp
from jax import lax
from jax.experimental import pallas as pl
from jax.experimental.pallas import tpu as pltpu
from jax.sharding import PartitionSpec as P

TILE = 384
B_SEND, B_PASS, B_HAVE, A_SEND, A_PASS, A_HAVE, MULT, SUM, A_OUT, LOAD_A, LOAD_B, NOTHING = range(12)
LETTERS = "bphafgmso"

END_ORDER = (
    "b00o10o31o11b01p00a70p01o30a40f70o20f40h01g70m71h00m70a60g40",
    "m41m40o21a50f60f50g60m61m60b02g50m51m50b03p02h02m62m72m42m52",
    "b04p03h03m63m73m43m53b05p04h04m64m74m44m54a30p05h05m65m75m45",
    "m55a10f30f10g30m35m34m33a20m32m31m30g10m15m14s14m13s13m12s12",
    "m11f20s11m10s10g20m25b06m24m23m22m21m20a00p06h06m66m76s15m46",
    "m56m26m36m16f00b07g00m06m05s05m04s04m03s03m02s02m01s01m00s00",
    "p07h07m67m77s06m47b08m57m27s16m37m07m17p08h08m68m78s07m48m58",
    "s17m28m38m08m18s08s18",
)
MID_ORDER = (
    "o31b00o01b01p00o30a00p01o21b02f00o00p02a60h00g00m00h01m01h02",
    "m02o20a50f60f50g60m60m61m62a70g50m50m51m52s61s60s01a10f70s51",
    "s00s50f10s62g70m70s70s02m71s71b03m72s72g10m10s10m11s52m12s11",
    "s12b04p03h03m63s63m73s73m53m03s53s03m13a40s13p04h04m64s64m74",
    "s74m54m04m14s04a30s54f40s14f30g40m40s40m41s41m42b05s42m43s43",
    "g30m30m44s44m31m32m33s33m34s34s32p05s31h05m65a20s65m75s30s75",
    "m45s45m55s55m35m05s05m15s15f20b06s35g20m20m21m22s22s21m23s23",
    "m24s24s20m25s25p06h06m66s66m76s76m46b07m56s46m26m36s56m06s06",
    "m16s16s26p07b08s36h07m67s67m77m47m57s77m27m37m07s07s47m17p08",
    "s17s57h08m68m78s27m48m58m28s37m38m08m18s68s78s08s48s18s58s28",
    "s38",
)


FIELDS = (4, 3, 4, 2, 2, 1, 1, 1, 1, 3, 4, 1, 1)
A_SLOTS, B_SLOTS, BLOCK = 4, 3, 16


def make_steps(order, own):
    text = "".join(order)
    ops = [(LETTERS.index(text[n]), int(text[n + 1]), int(text[n + 2])) for n in range(0, len(text), 3)]
    have = {op: n for n, op in enumerate(ops)}
    before = [[] for _ in ops]
    held = {LOAD_A: [None] * A_SLOTS, LOAD_B: [None] * B_SLOTS}
    used = {LOAD_A: [-1] * A_SLOTS, LOAD_B: [-1] * B_SLOTS}
    last = -1
    mults = {}
    for n, (op, g, j) in enumerate(ops):
        if op != MULT:
            continue
        wait, slot = {}, {}
        for load, what, ready in ((LOAD_B, j, have[(B_HAVE, 0, j)]), (LOAD_A, g, have[(A_HAVE, g, 0)])):
            wait[load] = int(what not in held[load])
            if wait[load]:
                slot[load] = used[load].index(min(used[load]))
                held[load][slot[load]] = what
                before[max(last, ready + 1)].append((load, g, j, slot[load]))
            else:
                slot[load] = held[load].index(what)
            used[load][slot[load]] = n
        mults[n] = (slot[LOAD_A], slot[LOAD_B], wait[LOAD_A], wait[LOAD_B])
        last = n
    steps = []
    pending, store = (0, 0, 0, 0, 0), 0

    def step(op, g, j, a_slot=0, b_slot=0, a_wait=0, b_wait=0, use=0):
        nonlocal pending
        steps.append((op, g, j, a_slot, b_slot, a_wait, b_wait, use, *pending))
        pending = (0, 0, 0, 0, 0)

    for n, (op, g, j) in enumerate(ops):
        for load, lg, lj, ls in before[n]:
            step(load, lg, lj, ls, ls)
        step(op, g, j, *mults.get(n, (0, 0, 0, 0)), store)
        if op == MULT or (op == SUM and g // 2 != own):
            pending = (1, g, j, store, int((op == MULT) == (own == 0) and g // 2 != own))
            store = 1 - store
    step(NOTHING, 0, 0)
    return steps


def choose(index, values):
    out = jnp.int32(values[-1])
    for k in range(len(values) - 2, -1, -1):
        out = jnp.where(index <= k, values[k], out)
    return out


def kernel(
    end_steps, mid_steps, a, b, c_out, a_all, b_all, part, low, high,
    mine, av, bv, acc, s0, s1, s2, cv,
    a1_s, a1_r, ax_s, ax_r, ay_s, ay_r, fx_s, fx_r, fy_s, fy_r,
    b_s, b_r, own_s, own_r, pass_s, pass_r, up_s, low_r, high_r, fin_s, fin_r, fin_l, lda, ldb, st, ls,
):
    rows, depth = a.shape[0], b.shape[0]
    tile = part.shape[3]
    tiles = part.shape[1]
    wide = tile * tiles
    half, quarter = rows // 2, rows // 4
    z, d = lax.axis_index("tp"), lax.axis_index("dp")
    q = d // 2
    core, x, y = d % 2, q % 2, d // 4
    q_x, q_y = q + 1 - 2 * x, q + 2 - 4 * y
    q_d = q_x + 2 - 4 * y
    peers = (q_x, q_y, q_d)

    def at(plane, chip):
        return {"tp": plane, "dp": chip * 2 + core}

    sibling = {"tp": z, "dp": d + 1 - 2 * core}

    def remote(src, dst, send, recv, to):
        return pltpu.make_async_remote_copy(
            src_ref=src, dst_ref=dst, send_sem=send, recv_sem=recv, device_id=to, device_id_type=pl.DeviceIdType.MESH
        )

    def a_rows(g, chip, first=0, count=half):
        return a_all.at[g, pl.ds(pl.multiple_of(chip * half + first, quarter), count), :]

    def b_rows(j, dev):
        return b_all.at[j, pl.ds(pl.multiple_of(dev * depth, depth), depth), :]

    def columns(chip, j):
        return pl.ds(pl.multiple_of(chip * wide + j * tile, tile), tile)

    def k_block(dev, plane):
        return pl.ds(pl.multiple_of((dev * 4 + plane) * depth, depth), depth)

    barrier = pltpu.get_barrier_semaphore()
    for plane in range(1, 4):
        pl.semaphore_signal(barrier, inc=1, device_id=at((z + plane) % 4, q), device_id_type=pl.DeviceIdType.MESH)
    for chip in peers:
        pl.semaphore_signal(barrier, inc=1, device_id=at(z, chip), device_id_type=pl.DeviceIdType.MESH)
    pl.semaphore_signal(barrier, inc=1, device_id=sibling, device_id_type=pl.DeviceIdType.MESH)
    pl.semaphore_wait(barrier, 7)

    def a_out(plane, h, dev):
        return remote(
            a.at[pl.ds(pl.multiple_of(h * half, half), half), k_block(dev, plane)],
            a_all.at[z * 2 + h, pl.ds(pl.multiple_of(q * half, half), half), pl.ds(pl.multiple_of(dev * depth, depth), depth)],
            a1_s.at[plane * 2 + h], a1_r.at[z * 2 + h], at(plane, q),
        )

    def own_in(dev):
        return pltpu.make_async_copy(a.at[:, k_block(dev, z)], mine.at[dev], lda.at[0, dev])

    def own_out(dev, h):
        return pltpu.make_async_copy(
            mine.at[dev, pl.ds(h * half, half), :],
            a_all.at[z * 2 + h, pl.ds(pl.multiple_of(q * half, half), half), pl.ds(pl.multiple_of(dev * depth, depth), depth)],
            ldb.at[h, dev],
        )

    @pl.loop(0, 8)
    def _(dev):
        own_in(dev).start()

    @pl.loop(0, 8)
    def _(dev):
        own_in(dev).wait()
        for h in range(2):
            own_out(dev, h).start()

    @pl.loop(0, 8)
    def _(dev):
        for h in range(2):
            own_out(dev, h).wait()

    def b_copy(j, n):
        return remote(b.at[:, columns(peers[n], j)], b_rows(j, d), b_s.at[j, n], b_r.at[j, n], at(z, peers[n]))

    def b_landed(j, n):
        dst = b_rows(j, peers[n] * 2 + core)
        return remote(dst, dst, b_s.at[j, n], b_r.at[j, n], at(z, peers[n]))

    def b_own(j):
        return remote(b.at[:, columns(q, j)], b_rows(j, d), own_s.at[j], own_r.at[j], sibling)

    def b_pass(j, n):
        dst = b_rows(j, peers[n] * 2 + core)
        return remote(dst, dst, pass_s.at[j, n], pass_r.at[j, n], sibling)

    def b_passed(j, n):
        dst = b_rows(j, peers[n] * 2 + 1 - core)
        return remote(dst, dst, pass_s.at[j, n], pass_r.at[j, n], sibling)

    def b_own_passed(j):
        dst = b_rows(j, d + 1 - 2 * core)
        return remote(dst, dst, own_s.at[j], own_r.at[j], sibling)

    def a_x(g, chip):
        return remote(a_rows(g, chip), a_rows(g, chip), ax_s.at[g], ax_r.at[g], at(z, q_x))

    def a_y(g, chip):
        return remote(a_rows(g, chip), a_rows(g, chip), ay_s.at[g], ay_r.at[g], at(z, q_y))

    def f_y(g, chip):
        return remote(a_rows(g, chip, 0, quarter), a_rows(g, chip, 0, quarter), fy_s.at[g], fy_r.at[g], at(z, q_y))

    def f_x(g, chip):
        return remote(a_rows(g, chip, quarter, quarter), a_rows(g, chip, quarter, quarter), fx_s.at[g], fx_r.at[g], at(z, q_x))

    def up(g, j):
        return remote(part.at[g, j], low.at[g, j], up_s.at[g, j], low_r.at[g, j], at(jnp.minimum(z + 1, 3), q))

    def down(g, j):
        return remote(part.at[g, j], high.at[g, j], up_s.at[g, j], high_r.at[g, j], at(jnp.maximum(z - 1, 0), q))

    def send_part(g, j):
        @pl.when(g // 2 > z)
        def _():
            up(g, j).start()

        @pl.when(g // 2 < z)
        def _():
            down(g, j).start()

    def final(h, j, n):
        return remote(
            cv.at[h, j, pl.ds(pl.multiple_of(peers[n] * half, half), half), :],
            c_out.at[pl.ds(pl.multiple_of(h * half, half), half), columns(q, j)],
            fin_s.at[h, j, n], fin_r.at[h, j, n], at(z, peers[n]),
        )

    def final_landed(h, j, n):
        dst = c_out.at[pl.ds(pl.multiple_of(h * half, half), half), columns(peers[n], j)]
        return remote(cv.at[h, j, pl.ds(0, half), :], dst, fin_s.at[h, j, n], fin_r.at[h, j, n], at(z, peers[n]))

    def final_own(h, j):
        return pltpu.make_async_copy(
            cv.at[h, j, pl.ds(pl.multiple_of(q * half, half), half), :],
            c_out.at[pl.ds(pl.multiple_of(h * half, half), half), columns(q, j)],
            fin_l.at[h, j],
        )

    def load_a(g, k, slot):
        dev = (d + k) % 8
        src = a_all.at[g, :, pl.ds(pl.multiple_of(dev * depth, depth), depth)]
        return pltpu.make_async_copy(src, av.at[slot, k], lda.at[slot, k])

    def load_b(j, k, slot):
        return pltpu.make_async_copy(b_rows(j, (d + k) % 8), bv.at[slot, k], ldb.at[slot, k])

    def load_b_own(j, slot):
        return pltpu.make_async_copy(b.at[:, columns(q, j)], bv.at[slot, 0], ldb.at[slot, 0])

    def stored(g, j, slot, sent):
        pltpu.make_async_copy(acc.at[slot], part.at[g, j], st.at[slot]).wait()

        @pl.when(sent == 1)
        def _():
            send_part(g, j)

    def multiply(g, j, a_slot, b_slot, a_wait, b_wait, use, settle):
        acc[use] = jnp.zeros(acc.shape[1:], acc.dtype)

        @pl.loop(0, 8, step=2)
        def _(k):
            for n in range(2):

                @pl.when(a_wait == 1)
                def _():
                    load_a(g, k + n, a_slot).wait()

                @pl.when(b_wait == 1)
                def _():
                    load_b(j, k + n, b_slot).wait()

            acc[use] += jnp.dot(av[a_slot, k], bv[b_slot, k], preferred_element_type=jnp.float32) + jnp.dot(
                av[a_slot, k + 1], bv[b_slot, k + 1], preferred_element_type=jnp.float32
            )

            @pl.when(k == 0)
            def _():
                settle()

        pltpu.make_async_copy(acc.at[use], part.at[g, j], st.at[use]).start()

    def add_up(g, j, use):
        i, h = g // 2, g % 2
        has_low = (z > 0) & (z <= i)
        has_high = (z < 3) & (z >= i)

        if True:
            mine = pltpu.make_async_copy(part.at[g, j], s0.at[use], ls.at[0])
            below = pltpu.make_async_copy(low.at[g, j], s1, ls.at[1])
            above = pltpu.make_async_copy(high.at[g, j], s2, ls.at[2])
            mine.start()

            @pl.when(has_low)
            def _():
                up(g, j).wait_recv()
                below.start()

            @pl.when(has_high)
            def _():
                down(g, j).wait_recv()
                above.start()

            mine.wait()

            @pl.when(has_low)
            def _():
                below.wait()
                s0[use] += s1[...]

            @pl.when(has_high)
            def _():
                above.wait()
                s0[use] += s2[...]

            @pl.when(i == z)
            def _():
                cv[h, j] = s0[use].astype(cv.dtype)
                for n in range(3):
                    final(h, j, n).start()
                final_own(h, j).start()

            @pl.when(i != z)
            def _():
                pltpu.make_async_copy(s0.at[use], part.at[g, j], st.at[use]).start()

    def run_step(code):
        fields = []
        for bits in FIELDS:
            fields.append(code % (1 << bits))
            code = code // (1 << bits)
        op, g, j, a_slot, b_slot, a_wait, b_wait, use, pending, last_g, last_j, last_use, sent = fields
        plane = jnp.where(z >= 2, 3 - g, g)
        g = jnp.where(z >= 2, 6 - g // 2 * 2 + g % 2, g)
        last_g = jnp.where(z >= 2, 6 - last_g // 2 * 2 + last_g % 2, last_g)

        def settle():
            @pl.when(pending == 1)
            def _():
                stored(last_g, last_j, last_use, sent)

        @pl.when(op != MULT)
        def _():
            settle()

        @pl.when(op == B_SEND)
        @jax.named_scope("b_send")
        def _():
            for n in range(3):
                b_copy(j, n).start()
            b_own(j).start()

        @pl.when(op == B_PASS)
        @jax.named_scope("b_pass")
        def _():
            for n in range(3):
                b_landed(j, n).wait_recv()
                b_pass(j, n).start()

        @pl.when(op == B_HAVE)
        @jax.named_scope("b_have")
        def _():
            b_own_passed(j).wait_recv()
            for n in range(3):
                b_passed(j, n).wait_recv()

        @pl.when(op == A_SEND)
        @jax.named_scope("a_send")
        def _():
            @pl.when(g // 2 != z)
            def _():
                landed = a_rows(g, q)
                remote(landed, landed, a1_s.at[0], a1_r.at[g], at(z, q_x)).wait_recv()

            a_x(g, q).start()
            a_y(g, q).start()

        @pl.when(op == A_PASS)
        @jax.named_scope("a_pass")
        def _():
            a_x(g, q_x).wait_recv()
            f_y(g, q_x).start()
            a_y(g, q_y).wait_recv()
            f_x(g, q_y).start()

        @pl.when(op == A_HAVE)
        @jax.named_scope("a_have")
        def _():
            f_y(g, q_d).wait_recv()
            f_x(g, q_d).wait_recv()

        @pl.when(op == A_OUT)
        def _():
            @pl.loop(0, 8)
            def _(dev):
                a_out(plane, j, dev).start()

        @pl.when(op == LOAD_A)
        def _():
            @pl.loop(0, 8)
            def _(k):
                load_a(g, k, a_slot).start()

        @pl.when(op == LOAD_B)
        def _():
            load_b_own(j, b_slot).start()

            @pl.loop(1, 8)
            def _(k):
                load_b(j, k, b_slot).start()

        @pl.when(op == MULT)
        @jax.named_scope("mult")
        def _():
            multiply(g, j, a_slot, b_slot, a_wait, b_wait, use, settle)

        @pl.when(op == SUM)
        @jax.named_scope("sum")
        def _():
            add_up(g, j, use)

    def codes(steps):
        packed = []
        for step in steps:
            code, at_bit = 0, 0
            for value, bits in zip(step, FIELDS, strict=True):
                code |= value << at_bit
                at_bit += bits
            packed.append(code)
        return packed

    end_codes, mid_codes = codes(end_steps), codes(mid_steps)
    blocks = -(-max(len(end_codes), len(mid_codes)) // BLOCK)
    table = [c + [NOTHING] * (blocks * BLOCK - len(c)) for c in (end_codes, mid_codes)]
    is_mid = jnp.where((z == 1) | (z == 2), blocks, 0)

    @pl.loop(0, blocks)
    def _(block):
        now = [choose(block + is_mid, [jnp.int32(v) for c in table for v in c[n::BLOCK]]) for n in range(BLOCK)]

        @pl.loop(0, BLOCK)
        def _(n):
            run_step(choose(n, now))

    @pl.loop(0, 8)
    def _(g):
        @pl.when(g // 2 != z)
        def _():
            remote(a_rows(g, q), a_rows(g, q), a1_s.at[g], a1_r.at[g], at(z, q_x)).wait_send()

        a_x(g, q).wait_send()
        a_y(g, q).wait_send()
        f_y(g, q_x).wait_send()
        f_x(g, q_y).wait_send()

        @pl.loop(0, tiles)
        def _(j):
            @pl.when(g // 2 != z)
            def _():
                up(g, j).wait_send()

    @pl.loop(0, tiles)
    def _(j):
        for n in range(3):
            b_copy(j, n).wait_send()
            b_pass(j, n).wait_send()
        b_own(j).wait_send()
        for h in range(2):
            for n in range(3):
                final_landed(h, j, n).wait_recv()
                final(h, j, n).wait_send()
            final_own(h, j).wait()


def solution(mesh):
    spec_rows = P(("dp", "tp"), None)

    def local_block(a, b):
        rows, depth, cols = a.shape[0], b.shape[0], b.shape[1]
        wide = cols // 4
        tile = min(TILE, wide // 9)
        tiles = wide // tile
        group = 2 * rows
        dma = pltpu.SemaphoreType.DMA
        any_space = pl.BlockSpec(memory_space=pl.ANY)
        out = pl.pallas_call(
            functools.partial(kernel, make_steps(END_ORDER, 0), make_steps(MID_ORDER, 1)),
            out_shape=[
                jax.ShapeDtypeStruct((rows, cols), jnp.bfloat16),
                jax.ShapeDtypeStruct((8, group, 8 * depth), jnp.bfloat16),
                jax.ShapeDtypeStruct((tiles, 8 * depth, tile), jnp.bfloat16),
                jax.ShapeDtypeStruct((8, tiles, group, tile), jnp.float32),
                jax.ShapeDtypeStruct((8, tiles, group, tile), jnp.float32),
                jax.ShapeDtypeStruct((8, tiles, group, tile), jnp.float32),
            ],
            in_specs=[any_space] * 2,
            out_specs=[any_space] * 6,
            scratch_shapes=[
                pltpu.VMEM((8, rows, depth), jnp.bfloat16),
                pltpu.VMEM((A_SLOTS, 8, group, depth), jnp.bfloat16),
                pltpu.VMEM((B_SLOTS, 8, depth, tile), jnp.bfloat16),
                pltpu.VMEM((2, group, tile), jnp.float32),
                pltpu.VMEM((2, group, tile), jnp.float32),
                pltpu.VMEM((group, tile), jnp.float32),
                pltpu.VMEM((group, tile), jnp.float32),
                pltpu.VMEM((2, tiles, group, tile), jnp.bfloat16),
                dma((8,)), dma((8,)),
                dma((8,)), dma((8,)), dma((8,)), dma((8,)),
                dma((8,)), dma((8,)), dma((8,)), dma((8,)),
                dma((tiles, 3)), dma((tiles, 3)), dma((tiles,)), dma((tiles,)), dma((tiles, 3)), dma((tiles, 3)),
                dma((8, tiles)), dma((8, tiles)), dma((8, tiles)),
                dma((2, tiles, 3)), dma((2, tiles, 3)), dma((2, tiles)),
                dma((A_SLOTS, 8)), dma((B_SLOTS, 8)), dma((2,)), dma((3,)),
            ],
            compiler_params=pltpu.CompilerParams(
                collective_id=0, has_side_effects=True, vmem_limit_bytes=60 * 1024 * 1024
            ),
        )(a, b)
        return out[0]

    return jax.shard_map(local_block, mesh=mesh, in_specs=(spec_rows, spec_rows), out_specs=spec_rows, check_vma=False)
```

```python
import functools

import jax
import jax.numpy as jnp
from jax import lax
from jax.experimental import pallas as pl
from jax.experimental.pallas import tpu as pltpu
from jax.sharding import PartitionSpec as P

TILE = 384
B_SEND, B_PASS, B_HAVE, A_SEND, A_PASS, A_HAVE, MULT, SUM, A_OUT, LOAD_A, LOAD_B, PUT, PUT_DONE, NOTHING = range(14)

END_ORDER = (
    0, 831, 370, 811, 100, 350, 470, 830, 820, 450, 810, 200, 570, 670, 1, 550, 650, 360, 101, 201, 671, 651, 340, 460,
    821, 440, 560, 661, 660, 2, 540, 641, 640, 3, 102, 202, 662, 672, 642, 652, 4, 103, 203, 663, 673, 643, 653, 5,
    104, 204, 664, 674, 644, 654, 320, 105, 205, 665, 675, 645, 655, 310, 420, 410, 520, 625, 624, 623, 6, 622, 621, 510,
    615, 620, 614, 613, 612, 611, 610, 710, 711, 106, 712, 713, 714, 206, 666, 7, 676, 626, 616, 646, 656, 8, 107, 207,
    667, 677, 627, 617, 647, 657, 300, 108, 208, 668, 678, 628, 618, 648, 715, 658, 400, 330, 716, 500, 608, 607, 606, 605,
    604, 603, 602, 601, 430, 600, 700, 701, 702, 703, 704, 705, 706, 707, 530, 638, 637, 636, 635, 634, 633, 632, 631, 630,
    717, 708, 718,
)
MID_ORDER = (
    831, 821, 800, 0, 830, 1, 100, 2, 101, 801, 3, 102, 820, 360, 103, 350, 460, 450, 200, 560, 660, 201, 661, 202,
    662, 300, 203, 663, 550, 650, 750, 651, 751, 652, 653, 761, 340, 400, 760, 440, 500, 600, 700, 762, 601, 370, 701, 540,
    640, 740, 641, 741, 642, 742, 643, 752, 602, 310, 702, 470, 603, 763, 743, 410, 753, 703, 570, 670, 770, 671, 4, 771,
    672, 772, 673, 773, 510, 610, 710, 611, 612, 711, 613, 712, 320, 104, 204, 644, 713, 744, 654, 754, 664, 764, 674, 5,
    774, 420, 604, 614, 704, 714, 105, 205, 645, 745, 6, 655, 755, 665, 765, 675, 775, 520, 620, 720, 621, 721, 622, 722,
    623, 723, 624, 106, 724, 625, 725, 206, 646, 7, 656, 666, 746, 766, 676, 776, 605, 705, 756, 615, 715, 626, 726, 606,
    107, 8, 706, 616, 716, 207, 647, 657, 667, 767, 677, 747, 777, 627, 330, 607, 108, 707, 757, 617, 208, 648, 727, 658,
    668, 717, 768, 678, 430, 778, 628, 608, 618, 708, 748, 530, 630, 631, 718, 758, 632, 633, 728, 634, 635, 636, 637, 737,
    638, 738, 736, 735, 734, 733, 732, 731, 730,
)


FIELDS = (4, 3, 4, 2, 2, 1, 1, 1, 1, 3, 4, 1, 1)
A_SLOTS, B_SLOTS, BLOCK = 4, 3, 16


def make_steps(order, own):
    ops = [(code // 100, code // 10 % 10, code % 10) for code in order]
    have = {op: n for n, op in enumerate(ops)}
    before = [[] for _ in ops]
    held = {LOAD_A: [None] * A_SLOTS, LOAD_B: [None] * B_SLOTS}
    used = {LOAD_A: [-1] * A_SLOTS, LOAD_B: [-1] * B_SLOTS}
    last = -1
    mults = {}
    for n, (op, g, j) in enumerate(ops):
        if op != MULT:
            continue
        wait, slot = {}, {}
        for load, what, ready in ((LOAD_B, j, have[(B_HAVE, 0, j)]), (LOAD_A, g, have[(A_HAVE, g, 0)])):
            wait[load] = int(what not in held[load])
            if wait[load]:
                slot[load] = used[load].index(min(used[load]))
                held[load][slot[load]] = what
                before[max(last, ready + 1)].append((load, g, j, slot[load]))
            else:
                slot[load] = held[load].index(what)
            used[load][slot[load]] = n
        mults[n] = (slot[LOAD_A], slot[LOAD_B], wait[LOAD_A], wait[LOAD_B])
        last = n
    steps = []
    pending, store = (0, 0, 0, 0, 0), 0
    first = next(n for n, op in enumerate(ops) if op[0] in (B_PASS, B_HAVE, A_SEND))

    def step(op, g, j, a_slot=0, b_slot=0, a_wait=0, b_wait=0, use=0):
        nonlocal pending
        steps.append((op, g, j, a_slot, b_slot, a_wait, b_wait, use, *pending))
        pending = (0, 0, 0, 0, 0)

    for n, (op, g, j) in enumerate(ops):
        for load, lg, lj, ls in before[n]:
            step(load, lg, lj, ls, ls)
        if n == first:
            step(PUT, 0, 0)
        if n == first + 1:
            step(PUT_DONE, 0, 0)
        step(op, g, j, *mults.get(n, (0, 0, 0, 0)), store)
        if op == MULT or (op == SUM and g // 2 != own):
            pending = (1, g, j, store, int((op == MULT) == (own == 0) and g // 2 != own))
            store = 1 - store
    step(NOTHING, 0, 0)
    return steps


def choose(index, values):
    out = jnp.int32(values[-1])
    for k in range(len(values) - 2, -1, -1):
        out = jnp.where(index <= k, values[k], out)
    return out


def kernel(
    end_steps, mid_steps, a, b, c_out, a_all, b_all, part, low, high,
    av, bv, acc, s0, s1, s2, cv,
    a1_s, a1_r, ax_s, ax_r, ay_s, ay_r, fx_s, fx_r, fy_s, fy_r,
    b_s, b_r, own_s, own_r, pass_s, pass_r, up_s, low_r, high_r, fin_s, fin_r, fin_l, lda, ldb, st, ls, put_s,
):
    rows, depth = a.shape[0], b.shape[0]
    tile = part.shape[3]
    tiles = part.shape[1]
    wide = tile * tiles
    half, quarter = rows // 2, rows // 4
    z, d = lax.axis_index("tp"), lax.axis_index("dp")
    q = d // 2
    core, x, y = d % 2, q % 2, d // 4
    q_x, q_y = q + 1 - 2 * x, q + 2 - 4 * y
    q_d = q_x + 2 - 4 * y
    peers = (q_x, q_y, q_d)

    def at(plane, chip):
        return {"tp": plane, "dp": chip * 2 + core}

    sibling = {"tp": z, "dp": d + 1 - 2 * core}

    def remote(src, dst, send, recv, to):
        return pltpu.make_async_remote_copy(
            src_ref=src, dst_ref=dst, send_sem=send, recv_sem=recv, device_id=to, device_id_type=pl.DeviceIdType.MESH
        )

    def a_rows(g, chip, first=0, count=half):
        return a_all.at[g, pl.ds(pl.multiple_of(chip * half + first, quarter), count), :]

    def b_rows(j, dev):
        return b_all.at[j, pl.ds(pl.multiple_of(dev * depth, depth), depth), :]

    def columns(chip, j):
        return pl.ds(pl.multiple_of(chip * wide + j * tile, tile), tile)

    def k_block(dev, plane):
        return pl.ds(pl.multiple_of((dev * 4 + plane) * depth, depth), depth)

    barrier = pltpu.get_barrier_semaphore()
    for plane in range(1, 4):
        pl.semaphore_signal(barrier, inc=1, device_id=at((z + plane) % 4, q), device_id_type=pl.DeviceIdType.MESH)
    for chip in peers:
        pl.semaphore_signal(barrier, inc=1, device_id=at(z, chip), device_id_type=pl.DeviceIdType.MESH)
    pl.semaphore_signal(barrier, inc=1, device_id=sibling, device_id_type=pl.DeviceIdType.MESH)
    pl.semaphore_wait(barrier, 7)

    def a_out(plane, h, dev):
        return remote(
            a.at[pl.ds(pl.multiple_of(h * half, half), half), k_block(dev, plane)],
            a_all.at[z * 2 + h, pl.ds(pl.multiple_of(q * half, half), half), pl.ds(pl.multiple_of(dev * depth, depth), depth)],
            a1_s.at[plane * 2 + h], a1_r.at[z * 2 + h], at(plane, q),
        )

    def own_in(dev):
        return pltpu.make_async_copy(
            a.at[:, k_block(dev, z)], av.at[0, pl.ds(0, rows), pl.ds(pl.multiple_of(dev * depth, depth), depth)], put_s.at[dev]
        )

    def own_out(h):
        return pltpu.make_async_copy(
            av.at[0, pl.ds(h * half, half), :],
            a_all.at[z * 2 + h, pl.ds(pl.multiple_of(q * half, half), half), :],
            put_s.at[h],
        )

    def b_spot(j):
        return bv.at[j // 8, pl.ds(pl.multiple_of(j % 8 * depth, depth), depth), :]

    def b_in(j):
        return pltpu.make_async_copy(b.at[:, columns(q, j)], b_spot(j), put_s.at[8 + j])

    def b_out(j):
        return pltpu.make_async_copy(b_spot(j), b_rows(j, d), put_s.at[8 + j])

    @pl.loop(0, 8)
    def _(dev):
        own_in(dev).start()

    @pl.loop(0, tiles)
    def _(j):
        b_in(j).start()

    def b_copy(j, n):
        return remote(b.at[:, columns(peers[n], j)], b_rows(j, d), b_s.at[j, n], b_r.at[j, n], at(z, peers[n]))

    def b_landed(j, n):
        dst = b_rows(j, peers[n] * 2 + core)
        return remote(dst, dst, b_s.at[j, n], b_r.at[j, n], at(z, peers[n]))

    def b_own(j):
        return remote(b.at[:, columns(q, j)], b_rows(j, d), own_s.at[j], own_r.at[j], sibling)

    def b_pass(j, n):
        dst = b_rows(j, peers[n] * 2 + core)
        return remote(dst, dst, pass_s.at[j, n], pass_r.at[j, n], sibling)

    def b_passed(j, n):
        dst = b_rows(j, peers[n] * 2 + 1 - core)
        return remote(dst, dst, pass_s.at[j, n], pass_r.at[j, n], sibling)

    def b_own_passed(j):
        dst = b_rows(j, d + 1 - 2 * core)
        return remote(dst, dst, own_s.at[j], own_r.at[j], sibling)

    def a_x(g, chip):
        return remote(a_rows(g, chip), a_rows(g, chip), ax_s.at[g], ax_r.at[g], at(z, q_x))

    def a_y(g, chip):
        return remote(a_rows(g, chip), a_rows(g, chip), ay_s.at[g], ay_r.at[g], at(z, q_y))

    def f_y(g, chip):
        return remote(a_rows(g, chip, 0, quarter), a_rows(g, chip, 0, quarter), fy_s.at[g], fy_r.at[g], at(z, q_y))

    def f_x(g, chip):
        return remote(a_rows(g, chip, quarter, quarter), a_rows(g, chip, quarter, quarter), fx_s.at[g], fx_r.at[g], at(z, q_x))

    def up(g, j):
        return remote(part.at[g, j], low.at[g, j], up_s.at[g, j], low_r.at[g, j], at(jnp.minimum(z + 1, 3), q))

    def down(g, j):
        return remote(part.at[g, j], high.at[g, j], up_s.at[g, j], high_r.at[g, j], at(jnp.maximum(z - 1, 0), q))

    def send_part(g, j):
        @pl.when(g // 2 > z)
        def _():
            up(g, j).start()

        @pl.when(g // 2 < z)
        def _():
            down(g, j).start()

    def final(h, j, n):
        return remote(
            cv.at[h, j, pl.ds(pl.multiple_of(peers[n] * half, half), half), :],
            c_out.at[pl.ds(pl.multiple_of(h * half, half), half), columns(q, j)],
            fin_s.at[h, j, n], fin_r.at[h, j, n], at(z, peers[n]),
        )

    def final_landed(h, j, n):
        dst = c_out.at[pl.ds(pl.multiple_of(h * half, half), half), columns(peers[n], j)]
        return remote(cv.at[h, j, pl.ds(0, half), :], dst, fin_s.at[h, j, n], fin_r.at[h, j, n], at(z, peers[n]))

    def final_own(h, j):
        return pltpu.make_async_copy(
            cv.at[h, j, pl.ds(pl.multiple_of(q * half, half), half), :],
            c_out.at[pl.ds(pl.multiple_of(h * half, half), half), columns(q, j)],
            fin_l.at[h, j],
        )

    def load_a(g, part_k, slot):
        span = pl.ds(part_k * 4 * depth, 4 * depth)
        return pltpu.make_async_copy(a_all.at[g, :, span], av.at[slot, :, span], lda.at[slot, part_k])

    def load_b(j, part_k, slot):
        span = pl.ds(part_k * 4 * depth, 4 * depth)
        return pltpu.make_async_copy(b_all.at[j, span, :], bv.at[slot, span, :], ldb.at[slot, part_k])

    def stored(g, j, slot, sent):
        pltpu.make_async_copy(acc.at[slot], part.at[g, j], st.at[slot]).wait()

        @pl.when(sent == 1)
        def _():
            send_part(g, j)

    def multiply(g, j, a_slot, b_slot, a_wait, b_wait, use, settle):
        for part_k in range(2):

            @pl.when(a_wait == 1)
            def _():
                load_a(g, part_k, a_slot).wait()

            @pl.when(b_wait == 1)
            def _():
                load_b(j, part_k, b_slot).wait()

            span = pl.ds(part_k * 4 * depth, 4 * depth)
            prod = jnp.dot(av[a_slot, :, span], bv[b_slot, span, :], preferred_element_type=jnp.float32)
            if part_k == 0:
                acc[use] = prod
                settle()
            else:
                acc[use] += prod

        pltpu.make_async_copy(acc.at[use], part.at[g, j], st.at[use]).start()

    def add_up(g, j, use, settle, same):
        i, h = g // 2, g % 2
        has_low = (z > 0) & (z <= i)
        has_high = (z < 3) & (z >= i)

        if True:
            mine = pltpu.make_async_copy(part.at[g, j], s0.at[use], ls.at[0])
            below = pltpu.make_async_copy(low.at[g, j], s1, ls.at[1])
            above = pltpu.make_async_copy(high.at[g, j], s2, ls.at[2])
            @pl.when(same)
            def _():
                settle()

            mine.start()

            @pl.when(jnp.logical_not(same))
            def _():
                settle()

            @pl.when(has_low)
            def _():
                up(g, j).wait_recv()
                below.start()

            @pl.when(has_high)
            def _():
                down(g, j).wait_recv()
                above.start()

            mine.wait()

            @pl.when(has_low)
            def _():
                below.wait()
                s0[use] += s1[...]

            @pl.when(has_high)
            def _():
                above.wait()
                s0[use] += s2[...]

            @pl.when(i == z)
            def _():
                cv[h, j] = s0[use].astype(cv.dtype)
                for n in range(3):
                    final(h, j, n).start()
                final_own(h, j).start()

            @pl.when(i != z)
            def _():
                pltpu.make_async_copy(s0.at[use], part.at[g, j], st.at[use]).start()

    def run_step(code):
        fields = []
        for bits in FIELDS:
            fields.append(code % (1 << bits))
            code = code // (1 << bits)
        op, g, j, a_slot, b_slot, a_wait, b_wait, use, pending, last_g, last_j, last_use, sent = fields
        plane = jnp.where(z >= 2, 3 - g, g)
        g = jnp.where(z >= 2, 6 - g // 2 * 2 + g % 2, g)
        last_g = jnp.where(z >= 2, 6 - last_g // 2 * 2 + last_g % 2, last_g)

        def settle():
            @pl.when(pending == 1)
            def _():
                stored(last_g, last_j, last_use, sent)

        @pl.when((op != MULT) & (op != SUM))
        def _():
            settle()

        @pl.when(op == B_SEND)
        @jax.named_scope("b_send")
        def _():
            for n in range(3):
                b_copy(j, n).start()
            b_own(j).start()

        @pl.when(op == B_PASS)
        @jax.named_scope("b_pass")
        def _():
            for n in range(3):
                b_landed(j, n).wait_recv()
                b_pass(j, n).start()

        @pl.when(op == B_HAVE)
        @jax.named_scope("b_have")
        def _():
            b_own_passed(j).wait_recv()
            for n in range(3):
                b_passed(j, n).wait_recv()

        @pl.when(op == A_SEND)
        @jax.named_scope("a_send")
        def _():
            @pl.when(g // 2 != z)
            def _():
                landed = a_rows(g, q)
                remote(landed, landed, a1_s.at[0], a1_r.at[g], at(z, q_x)).wait_recv()

            a_x(g, q).start()
            a_y(g, q).start()

        @pl.when(op == A_PASS)
        @jax.named_scope("a_pass")
        def _():
            a_x(g, q_x).wait_recv()
            f_y(g, q_x).start()
            a_y(g, q_y).wait_recv()
            f_x(g, q_y).start()

        @pl.when(op == A_HAVE)
        @jax.named_scope("a_have")
        def _():
            f_y(g, q_d).wait_recv()
            f_x(g, q_d).wait_recv()

        @pl.when(op == A_OUT)
        def _():
            @pl.loop(0, 8)
            def _(dev):
                a_out(plane, j, dev).start()

        @pl.when(op == LOAD_A)
        def _():
            for part_k in range(2):
                load_a(g, part_k, a_slot).start()

        @pl.when(op == LOAD_B)
        def _():
            for part_k in range(2):
                load_b(j, part_k, b_slot).start()

        @pl.when(op == PUT)
        def _():
            @pl.loop(0, 8)
            def _(dev):
                own_in(dev).wait()

            for h in range(2):
                own_out(h).start()

            @pl.loop(0, tiles)
            def _(n):
                b_in(n).wait()
                b_out(n).start()

        @pl.when(op == PUT_DONE)
        def _():
            for h in range(2):
                own_out(h).wait()

            @pl.loop(0, tiles)
            def _(n):
                b_out(n).wait()

        @pl.when(op == MULT)
        @jax.named_scope("mult")
        def _():
            multiply(g, j, a_slot, b_slot, a_wait, b_wait, use, settle)

        @pl.when(op == SUM)
        @jax.named_scope("sum")
        def _():
            add_up(g, j, use, settle, (last_g == g) & (last_j == j))

    def codes(steps):
        packed = []
        for step in steps:
            code, at_bit = 0, 0
            for value, bits in zip(step, FIELDS, strict=True):
                code |= value << at_bit
                at_bit += bits
            packed.append(code)
        return packed

    end_codes, mid_codes = codes(end_steps), codes(mid_steps)
    blocks = -(-max(len(end_codes), len(mid_codes)) // BLOCK)
    table = [c + [NOTHING] * (blocks * BLOCK - len(c)) for c in (end_codes, mid_codes)]
    is_mid = jnp.where((z == 1) | (z == 2), blocks, 0)

    @pl.loop(0, blocks)
    def _(block):
        now = [choose(block + is_mid, [jnp.int32(v) for c in table for v in c[n::BLOCK]]) for n in range(BLOCK)]

        @pl.loop(0, BLOCK)
        def _(n):
            run_step(choose(n, now))

    @pl.loop(0, 8)
    def _(g):
        @pl.when(g // 2 != z)
        def _():
            remote(a_rows(g, q), a_rows(g, q), a1_s.at[g], a1_r.at[g], at(z, q_x)).wait_send()

        a_x(g, q).wait_send()
        a_y(g, q).wait_send()
        f_y(g, q_x).wait_send()
        f_x(g, q_y).wait_send()

        @pl.loop(0, tiles)
        def _(j):
            @pl.when(g // 2 != z)
            def _():
                up(g, j).wait_send()

    @pl.loop(0, tiles)
    def _(j):
        for n in range(3):
            b_copy(j, n).wait_send()
            b_pass(j, n).wait_send()
        b_own(j).wait_send()
        for h in range(2):
            for n in range(3):
                final_landed(h, j, n).wait_recv()
                final(h, j, n).wait_send()
            final_own(h, j).wait()


def solution(mesh):
    spec_rows = P(("dp", "tp"), None)

    def local_block(a, b):
        rows, depth, cols = a.shape[0], b.shape[0], b.shape[1]
        wide = cols // 4
        tile = min(TILE, wide // 9)
        tiles = wide // tile
        group = 2 * rows
        dma = pltpu.SemaphoreType.DMA
        any_space = pl.BlockSpec(memory_space=pl.ANY)
        out = pl.pallas_call(
            functools.partial(kernel, make_steps(END_ORDER, 0), make_steps(MID_ORDER, 1)),
            out_shape=[
                jax.ShapeDtypeStruct((rows, cols), jnp.bfloat16),
                jax.ShapeDtypeStruct((8, group, 8 * depth), jnp.bfloat16),
                jax.ShapeDtypeStruct((tiles, 8 * depth, tile), jnp.bfloat16),
                jax.ShapeDtypeStruct((8, tiles, group, tile), jnp.float32),
                jax.ShapeDtypeStruct((8, tiles, group, tile), jnp.float32),
                jax.ShapeDtypeStruct((8, tiles, group, tile), jnp.float32),
            ],
            in_specs=[any_space] * 2,
            out_specs=[any_space] * 6,
            scratch_shapes=[
                pltpu.VMEM((A_SLOTS, group, 8 * depth), jnp.bfloat16),
                pltpu.VMEM((B_SLOTS, 8 * depth, tile), jnp.bfloat16),
                pltpu.VMEM((2, group, tile), jnp.float32),
                pltpu.VMEM((2, group, tile), jnp.float32),
                pltpu.VMEM((group, tile), jnp.float32),
                pltpu.VMEM((group, tile), jnp.float32),
                pltpu.VMEM((2, tiles, group, tile), jnp.bfloat16),
                dma((8,)), dma((8,)),
                dma((8,)), dma((8,)), dma((8,)), dma((8,)),
                dma((8,)), dma((8,)), dma((8,)), dma((8,)),
                dma((tiles, 3)), dma((tiles, 3)), dma((tiles,)), dma((tiles,)), dma((tiles, 3)), dma((tiles, 3)),
                dma((8, tiles)), dma((8, tiles)), dma((8, tiles)),
                dma((2, tiles, 3)), dma((2, tiles, 3)), dma((2, tiles)),
                dma((A_SLOTS, 2)), dma((B_SLOTS, 2)), dma((2,)), dma((3,)), dma((8 + tiles,)),
            ],
            compiler_params=pltpu.CompilerParams(
                collective_id=0, has_side_effects=True, vmem_limit_bytes=60 * 1024 * 1024
            ),
        )(a, b)
        return out[0]

    return jax.shard_map(local_block, mesh=mesh, in_specs=(spec_rows, spec_rows), out_specs=spec_rows, check_vma=False)
```

```python
import functools

import jax
import jax.numpy as jnp
from jax import lax
from jax.experimental import pallas as pl
from jax.experimental.pallas import tpu as pltpu
from jax.sharding import PartitionSpec as P

TILE = 384
B_SEND, B_PASS, B_HAVE, A_SEND, A_PASS, A_HAVE, MULT, SUM, A_OUT, LOAD_A, LOAD_B, PUT, PUT_DONE, NOTHING = range(14)

END_ORDER = (
    911100920930450200910101, 550201460301650751300750, 931420560921520660761760, 102620721720103202302762,
    752722470203303763753723, 570104670773772771770105, 204304764774754724440205, 305765775755725540106640,
    745744743742741740400206, 306766776746756726500430, 600706705805704804703803, 702802701530801700800630,
    736107735734733732731730, 410207806307767777747757, 727737510707108610717716, 816715815714814713813712,
    812711208811710810308768, 778748758807728738817708, 718808818,
)
MID_ORDER = (
    901931900921100920101200, 460201102560202400300660, 760301761302762450500550, 861600700860701470801702,
    650750850800751851752862, 103570852802203303763410, 863753930853670770771772, 773873703803510872104871,
    610710711870712713813812, 105204811304764864774810, 874754854704804440714814, 205305765865775875755855,
    705805540715815420640740, 741742743843744842844745, 520845841106840620720721, 722822723823724824725821,
    825206306766430820866776, 876726746846756856706806, 716530816826107630730731, 732832733833734831834735,
    835830736207836307767867, 777108877727737747847757, 707857807717817827208308, 768837778728868738748878,
    758708808848718818858828, 838,
)


FIELDS = (4, 3, 4, 2, 2, 1, 1, 1, 1, 3, 4, 1, 1)
A_SLOTS, B_SLOTS, BLOCK = 4, 3, 16


def make_steps(order, own):
    text = "".join(map(str, order))
    ops = [(int(text[n]) - 1, int(text[n + 1]), int(text[n + 2])) for n in range(0, len(text), 3)]
    have = {op: n for n, op in enumerate(ops)}
    before = [[] for _ in ops]
    held = {LOAD_A: [None] * A_SLOTS, LOAD_B: [None] * B_SLOTS}
    used = {LOAD_A: [-1] * A_SLOTS, LOAD_B: [-1] * B_SLOTS}
    last = -1
    mults = {}
    for n, (op, g, j) in enumerate(ops):
        if op != MULT:
            continue
        wait, slot = {}, {}
        for load, what, ready in ((LOAD_B, j, have[(B_HAVE, 0, j)]), (LOAD_A, g, have[(A_HAVE, g, 0)])):
            wait[load] = int(what not in held[load])
            if wait[load]:
                slot[load] = used[load].index(min(used[load]))
                held[load][slot[load]] = what
                before[max(last, ready + 1)].append((load, g, j, slot[load]))
            else:
                slot[load] = held[load].index(what)
            used[load][slot[load]] = n
        mults[n] = (slot[LOAD_A], slot[LOAD_B], wait[LOAD_A], wait[LOAD_B])
        last = n
    steps = []
    pending, store = (0, 0, 0, 0, 0), 0
    first = next(n for n, op in enumerate(ops) if op[0] in (B_PASS, B_HAVE, A_SEND))

    def step(op, g, j, a_slot=0, b_slot=0, a_wait=0, b_wait=0, use=0):
        nonlocal pending
        steps.append((op, g, j, a_slot, b_slot, a_wait, b_wait, use, *pending))
        pending = (0, 0, 0, 0, 0)

    for n, (op, g, j) in enumerate(ops):
        for load, lg, lj, ls in before[n]:
            step(load, lg, lj, ls, ls)
        if n == first:
            step(PUT, 0, 0)
        if n == first + 1:
            step(PUT_DONE, 0, 0)
        step(op, g, j, *mults.get(n, (0, 0, 0, 0)), store)
        if op == MULT or (op == SUM and g // 2 != own):
            pending = (1, g, j, store, int((op == MULT) == (own == 0) and g // 2 != own))
            store = 1 - store
    step(NOTHING, 0, 0)
    return steps


def choose(index, values):
    out = jnp.int32(values[-1])
    for k in range(len(values) - 2, -1, -1):
        out = jnp.where(index <= k, values[k], out)
    return out


def kernel(
    end_steps, mid_steps, a, b, c_out, a_all, b_all, part, low, high,
    av, bv, acc, s0, s1, s2, cv,
    a1_s, a1_r, a_s, ax_r, ay_r, fx_r, fy_r,
    b_s, b_r, own_s, own_r, pass_s, pass_r, up_s, low_r, high_r, fin_s, fin_r, fin_l, lda, ldb, st, ls, put_s,
):
    rows, depth = a.shape[0], b.shape[0]
    tile = part.shape[3]
    tiles = part.shape[1]
    wide = tile * tiles
    half, quarter = rows // 2, rows // 4
    z, d = lax.axis_index("tp"), lax.axis_index("dp")
    q = d // 2
    core, x, y = d % 2, q % 2, d // 4
    q_x, q_y = q + 1 - 2 * x, q + 2 - 4 * y
    q_d = q_x + 2 - 4 * y
    peers = (q_x, q_y, q_d)

    def at(plane, chip):
        return {"tp": plane, "dp": chip * 2 + core}

    sibling = {"tp": z, "dp": d + 1 - 2 * core}

    def remote(src, dst, send, recv, to):
        return pltpu.make_async_remote_copy(
            src_ref=src, dst_ref=dst, send_sem=send, recv_sem=recv, device_id=to, device_id_type=pl.DeviceIdType.MESH
        )

    def a_rows(g, chip, first=0, count=half):
        return a_all.at[g, pl.ds(pl.multiple_of(chip * half + first, quarter), count), :]

    def b_rows(j, dev):
        return b_all.at[j, pl.ds(pl.multiple_of(dev * depth, depth), depth), :]

    def columns(chip, j):
        return pl.ds(pl.multiple_of(chip * wide + j * tile, tile), tile)

    def k_block(dev, plane):
        return pl.ds(pl.multiple_of((dev * 4 + plane) * depth, depth), depth)

    barrier = pltpu.get_barrier_semaphore()
    for plane in range(1, 4):
        pl.semaphore_signal(barrier, inc=1, device_id=at((z + plane) % 4, q), device_id_type=pl.DeviceIdType.MESH)
    for chip in peers:
        pl.semaphore_signal(barrier, inc=1, device_id=at(z, chip), device_id_type=pl.DeviceIdType.MESH)
    pl.semaphore_signal(barrier, inc=1, device_id=sibling, device_id_type=pl.DeviceIdType.MESH)
    pl.semaphore_wait(barrier, 7)

    def a_out(plane, h, dev):
        return remote(
            a.at[pl.ds(pl.multiple_of(h * half, half), half), k_block(dev, plane)],
            a_all.at[z * 2 + h, pl.ds(pl.multiple_of(q * half, half), half), pl.ds(pl.multiple_of(dev * depth, depth), depth)],
            a1_s, a1_r.at[z * 2 + h], at(plane, q),
        )

    def own_in(dev):
        return pltpu.make_async_copy(
            a.at[:, k_block(dev, z)], av.at[0, pl.ds(0, rows), pl.ds(pl.multiple_of(dev * depth, depth), depth)], put_s.at[dev]
        )

    def own_out(h):
        return pltpu.make_async_copy(
            av.at[0, pl.ds(h * half, half), :],
            a_all.at[z * 2 + h, pl.ds(pl.multiple_of(q * half, half), half), :],
            put_s.at[h],
        )

    def b_spot(j):
        return bv.at[j // 8, pl.ds(pl.multiple_of(j % 8 * depth, depth), depth), :]

    def b_in(j):
        return pltpu.make_async_copy(b.at[:, columns(q, j)], b_spot(j), put_s.at[8 + j])

    def b_out(j):
        return pltpu.make_async_copy(b_spot(j), b_rows(j, d), put_s.at[8 + j])

    @pl.loop(0, 8)
    def _(dev):
        own_in(dev).start()

    @pl.loop(0, tiles)
    def _(j):
        b_in(j).start()

    def b_copy(j, n):
        return remote(b.at[:, columns(peers[n], j)], b_rows(j, d), b_s, b_r.at[j, n], at(z, peers[n]))

    def b_landed(j, n):
        dst = b_rows(j, peers[n] * 2 + core)
        return remote(dst, dst, b_s, b_r.at[j, n], at(z, peers[n]))

    def b_own(j):
        return remote(b.at[:, columns(q, j)], b_rows(j, d), own_s, own_r.at[j], sibling)

    def b_pass(j, n):
        dst = b_rows(j, peers[n] * 2 + core)
        return remote(dst, dst, pass_s, pass_r.at[j, n], sibling)

    def b_passed(j, n):
        dst = b_rows(j, peers[n] * 2 + 1 - core)
        return remote(dst, dst, pass_s, pass_r.at[j, n], sibling)

    def b_own_passed(j):
        dst = b_rows(j, d + 1 - 2 * core)
        return remote(dst, dst, own_s, own_r.at[j], sibling)

    def a_x(g, chip):
        return remote(a_rows(g, chip), a_rows(g, chip), a_s, ax_r.at[g], at(z, q_x))

    def a_y(g, chip):
        return remote(a_rows(g, chip), a_rows(g, chip), a_s, ay_r.at[g], at(z, q_y))

    def f_y(g, chip):
        return remote(a_rows(g, chip, 0, quarter), a_rows(g, chip, 0, quarter), a_s, fy_r.at[g], at(z, q_y))

    def f_x(g, chip):
        return remote(a_rows(g, chip, quarter, quarter), a_rows(g, chip, quarter, quarter), a_s, fx_r.at[g], at(z, q_x))

    def up(g, j):
        return remote(part.at[g, j], low.at[g, j], up_s, low_r.at[g, j], at(jnp.minimum(z + 1, 3), q))

    def down(g, j):
        return remote(part.at[g, j], high.at[g, j], up_s, high_r.at[g, j], at(jnp.maximum(z - 1, 0), q))

    def send_part(g, j):
        @pl.when(g // 2 > z)
        def _():
            up(g, j).start()

        @pl.when(g // 2 < z)
        def _():
            down(g, j).start()

    def final(h, j, n):
        return remote(
            cv.at[h, j, pl.ds(pl.multiple_of(peers[n] * half, half), half), :],
            c_out.at[pl.ds(pl.multiple_of(h * half, half), half), columns(q, j)],
            fin_s, fin_r, at(z, peers[n]),
        )

    def final_own(h, j):
        return pltpu.make_async_copy(
            cv.at[h, j, pl.ds(pl.multiple_of(q * half, half), half), :],
            c_out.at[pl.ds(pl.multiple_of(h * half, half), half), columns(q, j)],
            fin_l,
        )

    def load_a(g, part_k, slot):
        span = pl.ds(part_k * 4 * depth, 4 * depth)
        return pltpu.make_async_copy(a_all.at[g, :, span], av.at[slot, :, span], lda.at[slot, part_k])

    def load_b(j, part_k, slot):
        span = pl.ds(part_k * 4 * depth, 4 * depth)
        return pltpu.make_async_copy(b_all.at[j, span, :], bv.at[slot, span, :], ldb.at[slot, part_k])

    def stored(g, j, slot, sent):
        pltpu.make_async_copy(acc.at[slot], part.at[g, j], st.at[slot]).wait()

        @pl.when(sent == 1)
        def _():
            send_part(g, j)

    def multiply(g, j, a_slot, b_slot, a_wait, b_wait, use, settle):
        for part_k in range(2):

            @pl.when(a_wait == 1)
            def _():
                load_a(g, part_k, a_slot).wait()

            @pl.when(b_wait == 1)
            def _():
                load_b(j, part_k, b_slot).wait()

            span = pl.ds(part_k * 4 * depth, 4 * depth)
            prod = jnp.dot(av[a_slot, :, span], bv[b_slot, span, :], preferred_element_type=jnp.float32)
            if part_k == 0:
                acc[use] = prod
                settle()
            else:
                acc[use] += prod

        pltpu.make_async_copy(acc.at[use], part.at[g, j], st.at[use]).start()

    def add_up(g, j, use, settle, same):
        i, h = g // 2, g % 2
        has_low = (z > 0) & (z <= i)
        has_high = (z < 3) & (z >= i)

        if True:
            mine = pltpu.make_async_copy(part.at[g, j], s0.at[use], ls.at[0])
            below = pltpu.make_async_copy(low.at[g, j], s1, ls.at[1])
            above = pltpu.make_async_copy(high.at[g, j], s2, ls.at[2])
            @pl.when(same)
            def _():
                settle()

            mine.start()

            @pl.when(jnp.logical_not(same))
            def _():
                settle()

            @pl.when(has_low)
            def _():
                up(g, j).wait_recv()
                below.start()

            @pl.when(has_high)
            def _():
                down(g, j).wait_recv()
                above.start()

            mine.wait()

            @pl.when(has_low)
            def _():
                below.wait()
                s0[use] += s1[...]

            @pl.when(has_high)
            def _():
                above.wait()
                s0[use] += s2[...]

            @pl.when(i == z)
            def _():
                cv[h, j] = s0[use].astype(cv.dtype)
                for n in range(3):
                    final(h, j, n).start()
                final_own(h, j).start()

            @pl.when(i != z)
            def _():
                pltpu.make_async_copy(s0.at[use], part.at[g, j], st.at[use]).start()

    def run_step(code):
        fields = []
        for bits in FIELDS:
            fields.append(code % (1 << bits))
            code = code // (1 << bits)
        op, g, j, a_slot, b_slot, a_wait, b_wait, use, pending, last_g, last_j, last_use, sent = fields
        plane = jnp.where(z >= 2, 3 - g, g)
        g = jnp.where(z >= 2, 6 - g // 2 * 2 + g % 2, g)
        last_g = jnp.where(z >= 2, 6 - last_g // 2 * 2 + last_g % 2, last_g)

        def settle():
            @pl.when(pending == 1)
            def _():
                stored(last_g, last_j, last_use, sent)

        @pl.when((op != MULT) & (op != SUM))
        def _():
            settle()

        @pl.when(op == B_SEND)
        @jax.named_scope("b_send")
        def _():
            for n in range(3):
                b_copy(j, n).start()
            b_own(j).start()

        @pl.when(op == B_PASS)
        @jax.named_scope("b_pass")
        def _():
            for n in range(3):
                b_landed(j, n).wait_recv()
                b_pass(j, n).start()

        @pl.when(op == B_HAVE)
        @jax.named_scope("b_have")
        def _():
            b_own_passed(j).wait_recv()
            for n in range(3):
                b_passed(j, n).wait_recv()

        @pl.when(op == A_SEND)
        @jax.named_scope("a_send")
        def _():
            @pl.when(g // 2 != z)
            def _():
                landed = a_rows(g, q)
                remote(landed, landed, a1_s, a1_r.at[g], at(z, q_x)).wait_recv()

            a_x(g, q).start()
            a_y(g, q).start()

        @pl.when(op == A_PASS)
        @jax.named_scope("a_pass")
        def _():
            a_x(g, q_x).wait_recv()
            f_y(g, q_x).start()
            a_y(g, q_y).wait_recv()
            f_x(g, q_y).start()

        @pl.when(op == A_HAVE)
        @jax.named_scope("a_have")
        def _():
            f_y(g, q_d).wait_recv()
            f_x(g, q_d).wait_recv()

        @pl.when(op == A_OUT)
        def _():
            @pl.loop(0, 8)
            def _(dev):
                a_out(plane, j, dev).start()

        @pl.when(op == LOAD_A)
        def _():
            for part_k in range(2):
                load_a(g, part_k, a_slot).start()

        @pl.when(op == LOAD_B)
        def _():
            for part_k in range(2):
                load_b(j, part_k, b_slot).start()

        @pl.when(op == PUT)
        def _():
            @pl.loop(0, 8)
            def _(dev):
                own_in(dev).wait()

            for h in range(2):
                own_out(h).start()

            @pl.loop(0, tiles)
            def _(n):
                b_in(n).wait()
                b_out(n).start()

        @pl.when(op == PUT_DONE)
        def _():
            for h in range(2):
                own_out(h).wait()

            @pl.loop(0, tiles)
            def _(n):
                b_out(n).wait()

        @pl.when(op == MULT)
        @jax.named_scope("mult")
        def _():
            multiply(g, j, a_slot, b_slot, a_wait, b_wait, use, settle)

        @pl.when(op == SUM)
        @jax.named_scope("sum")
        def _():
            add_up(g, j, use, settle, (last_g == g) & (last_j == j))

    def codes(steps):
        packed = []
        for step in steps:
            code, at_bit = 0, 0
            for value, bits in zip(step, FIELDS, strict=True):
                code |= value << at_bit
                at_bit += bits
            packed.append(code)
        return packed

    end_codes, mid_codes = codes(end_steps), codes(mid_steps)
    blocks = -(-max(len(end_codes), len(mid_codes)) // BLOCK)
    table = [c + [NOTHING] * (blocks * BLOCK - len(c)) for c in (end_codes, mid_codes)]
    is_mid = jnp.where((z == 1) | (z == 2), blocks, 0)

    @pl.loop(0, blocks)
    def _(block):
        now = [choose(block + is_mid, [jnp.int32(v) for c in table for v in c[n::BLOCK]]) for n in range(BLOCK)]

        @pl.loop(0, BLOCK)
        def _(n):
            run_step(choose(n, now))

    def all_done(like, sem):
        pltpu.make_async_copy(like, like, sem).wait()

    with jax.named_scope("drain"):
        for sem, count in ((b_s, 3), (pass_s, 3), (own_s, 1)):
            all_done(b.at[:, pl.ds(0, count * wide)], sem)
        all_done(a.at[:, pl.ds(0, 24 * depth)], a1_s)
        all_done(a_all.at[pl.ds(0, 6)], a_s)
        all_done(c_out.at[:, pl.ds(0, wide)], fin_l)
        all_done(part.at[pl.ds(0, 6)], up_s)
        for sem in (fin_s, fin_r):
            all_done(c_out.at[:, pl.ds(0, 3 * wide)], sem)


def solution(mesh):
    spec_rows = P(("dp", "tp"), None)

    def local_block(a, b):
        rows, depth, cols = a.shape[0], b.shape[0], b.shape[1]
        wide = cols // 4
        tile = min(TILE, wide // 9)
        tiles = wide // tile
        group = 2 * rows
        dma = pltpu.SemaphoreType.DMA
        any_space = pl.BlockSpec(memory_space=pl.ANY)
        out = pl.pallas_call(
            functools.partial(kernel, make_steps(END_ORDER, 0), make_steps(MID_ORDER, 1)),
            out_shape=[
                jax.ShapeDtypeStruct((rows, cols), jnp.bfloat16),
                jax.ShapeDtypeStruct((8, group, 8 * depth), jnp.bfloat16),
                jax.ShapeDtypeStruct((tiles, 8 * depth, tile), jnp.bfloat16),
                jax.ShapeDtypeStruct((8, tiles, group, tile), jnp.float32),
                jax.ShapeDtypeStruct((8, tiles, group, tile), jnp.float32),
                jax.ShapeDtypeStruct((8, tiles, group, tile), jnp.float32),
            ],
            in_specs=[any_space] * 2,
            out_specs=[any_space] * 6,
            scratch_shapes=[
                pltpu.VMEM((A_SLOTS, group, 8 * depth), jnp.bfloat16),
                pltpu.VMEM((B_SLOTS, 8 * depth, tile), jnp.bfloat16),
                pltpu.VMEM((2, group, tile), jnp.float32),
                pltpu.VMEM((2, group, tile), jnp.float32),
                pltpu.VMEM((group, tile), jnp.float32),
                pltpu.VMEM((group, tile), jnp.float32),
                pltpu.VMEM((2, tiles, group, tile), jnp.bfloat16),
                dma, dma((8,)), dma, dma((8,)), dma((8,)), dma((8,)), dma((8,)),
                dma, dma((tiles, 3)), dma, dma((tiles,)), dma, dma((tiles, 3)),
                dma, dma((8, tiles)), dma((8, tiles)), dma, dma, dma,
                dma((A_SLOTS, 2)), dma((B_SLOTS, 2)), dma((2,)), dma((3,)), dma((8 + tiles,)),
            ],
            compiler_params=pltpu.CompilerParams(
                collective_id=0, has_side_effects=True, vmem_limit_bytes=60 * 1024 * 1024
            ),
        )(a, b)
        return out[0]

    return jax.shard_map(local_block, mesh=mesh, in_specs=(spec_rows, spec_rows), out_specs=spec_rows, check_vma=False)
```

```python
import functools

import jax
import jax.numpy as jnp
from jax import lax
from jax.experimental import pallas as pl
from jax.experimental.pallas import tpu as pltpu
from jax.sharding import PartitionSpec as P

TILE = 384
B_SEND, B_PASS, B_HAVE, A_SEND, A_PASS, A_HAVE, MULT, SUM, A_OUT, LOAD_A, LOAD_B, PUT, PUT_DONE, NOTHING = range(14)

END_ORDER = (
    100920910430200930931101, 530201460301630731300730, 921911470560570660761760, 102670771770103202302732,
    762772440203303733763773, 540104640743742741740450, 204304734744764774550105, 650754753752751750106205,
    305735745755765775400206, 306736746756766776500107, 600706705704703702701700, 804803802801207800307707,
    737108747757767777805208, 420308708738748758768778, 806520410620728727726725, 724723722721510720807610,
    718717716715714713712711, 710808818817816815814813, 812811810,
)
MID_ORDER = (
    920930901100931101200900, 102201400202921500460300, 600700301701302702470560, 570660760860761103861762,
    670770870800771871801772, 440862203303763872773802, 703540863410873803640740, 741742743843842510841104,
    610710840810711811712812, 713813450204304744844764, 864774874704714550804105, 814650750751851752852753,
    853850754430854205305745, 845755765855775705865530, 715875106630730830731831, 732832733805833734834815,
    735206835306746107846756, 856736766866776876706836, 716108806207307747847757, 857816737767867777420877,
    837707208717308748848758, 858807817738768520868778, 878708838718620720808721, 722818723724725825726826,
    727827824728828823822821, 820,
)


FIELDS = (4, 3, 4, 2, 2, 1, 1, 1, 1, 3, 4, 1, 1)
A_SLOTS, B_SLOTS, BLOCK = 4, 3, 16


def make_steps(order, own):
    text = "".join(map(str, order))
    ops = [(int(text[n]) - 1, int(text[n + 1]), int(text[n + 2])) for n in range(0, len(text), 3)]
    have = {op: n for n, op in enumerate(ops)}
    before = [[] for _ in ops]
    held = {LOAD_A: [None] * A_SLOTS, LOAD_B: [None] * B_SLOTS}
    used = {LOAD_A: [-1] * A_SLOTS, LOAD_B: [-1] * B_SLOTS}
    last = -1
    mults = {}
    for n, (op, g, j) in enumerate(ops):
        if op != MULT:
            continue
        wait, slot = {}, {}
        for load, what, ready in ((LOAD_B, j, have[(B_HAVE, 0, j)]), (LOAD_A, g, have[(A_HAVE, g, 0)])):
            wait[load] = int(what not in held[load])
            if wait[load]:
                slot[load] = used[load].index(min(used[load]))
                held[load][slot[load]] = what
                before[max(last, ready + 1)].append((load, g, j, slot[load]))
            else:
                slot[load] = held[load].index(what)
            used[load][slot[load]] = n
        mults[n] = (slot[LOAD_A], slot[LOAD_B], wait[LOAD_A], wait[LOAD_B])
        last = n
    steps = []
    pending, store = (0, 0, 0, 0, 0), 0
    first = next(n for n, op in enumerate(ops) if op[0] in (B_PASS, B_HAVE, A_SEND))

    def step(op, g, j, a_slot=0, b_slot=0, a_wait=0, b_wait=0, use=0):
        nonlocal pending
        steps.append((op, g, j, a_slot, b_slot, a_wait, b_wait, use, *pending))
        pending = (0, 0, 0, 0, 0)

    for n, (op, g, j) in enumerate(ops):
        for load, lg, lj, ls in before[n]:
            step(load, lg, lj, ls, ls)
        if n == first:
            step(PUT, 0, 0)
        if n == first + 1:
            step(PUT_DONE, 0, 0)
        step(op, g, j, *mults.get(n, (0, 0, 0, 0)), store)
        if op == MULT or (op == SUM and g // 2 != own):
            pending = (1, g, j, store, int((op == MULT) == (own == 0) and g // 2 != own))
            store = 1 - store
    step(NOTHING, 0, 0)
    return steps


def choose(index, values):
    out = jnp.int32(values[-1])
    for k in range(len(values) - 2, -1, -1):
        out = jnp.where(index <= k, values[k], out)
    return out


def kernel(
    end_steps, mid_steps, a, b, c_out, a_all, b_all, part, low, high,
    av, bv, acc, s0, s1, s2, cv,
    a1_s, a1_r, a_s, ax_r, ay_r, fx_r, fy_r,
    b_s, b_r, own_s, own_r, pass_s, pass_r, up_s, low_r, high_r, fin_s, fin_r, fin_l, lda, ldb, st, ls, put_s,
):
    rows, depth = a.shape[0], b.shape[0]
    tile = part.shape[3]
    tiles = part.shape[1]
    wide = tile * tiles
    half, quarter = rows // 2, rows // 4
    z, d = lax.axis_index("tp"), lax.axis_index("dp")
    q = d // 2
    core, x, y = d % 2, q % 2, d // 4
    q_x, q_y = q + 1 - 2 * x, q + 2 - 4 * y
    q_d = q_x + 2 - 4 * y
    peers = (q_x, q_y, q_d)

    def at(plane, chip):
        return {"tp": plane, "dp": chip * 2 + core}

    sibling = {"tp": z, "dp": d + 1 - 2 * core}

    def remote(src, dst, send, recv, to):
        return pltpu.make_async_remote_copy(
            src_ref=src, dst_ref=dst, send_sem=send, recv_sem=recv, device_id=to, device_id_type=pl.DeviceIdType.MESH
        )

    def a_rows(g, chip, first=0, count=half):
        return a_all.at[g, pl.ds(pl.multiple_of(chip * half + first, quarter), count), :]

    def b_rows(j, dev):
        return b_all.at[j, pl.ds(pl.multiple_of(dev * depth, depth), depth), :]

    def columns(chip, j):
        return pl.ds(pl.multiple_of(chip * wide + j * tile, tile), tile)

    def k_block(dev, plane):
        return pl.ds(pl.multiple_of((dev * 4 + plane) * depth, depth), depth)

    barrier = pltpu.get_barrier_semaphore()
    for plane in range(1, 4):
        pl.semaphore_signal(barrier, inc=1, device_id=at((z + plane) % 4, q), device_id_type=pl.DeviceIdType.MESH)
    for chip in peers:
        pl.semaphore_signal(barrier, inc=1, device_id=at(z, chip), device_id_type=pl.DeviceIdType.MESH)
    pl.semaphore_signal(barrier, inc=1, device_id=sibling, device_id_type=pl.DeviceIdType.MESH)
    pl.semaphore_wait(barrier, 7)

    def a_out(plane, h, dev):
        return remote(
            a.at[pl.ds(pl.multiple_of(h * half, half), half), k_block(dev, plane)],
            a_all.at[z * 2 + h, pl.ds(pl.multiple_of(q * half, half), half), pl.ds(pl.multiple_of(dev * depth, depth), depth)],
            a1_s, a1_r.at[z * 2 + h], at(plane, q),
        )

    def own_in(dev):
        return pltpu.make_async_copy(
            a.at[:, k_block(dev, z)], av.at[0, pl.ds(0, rows), pl.ds(pl.multiple_of(dev * depth, depth), depth)], put_s.at[dev]
        )

    def own_out(h):
        return pltpu.make_async_copy(
            av.at[0, pl.ds(h * half, half), :],
            a_all.at[z * 2 + h, pl.ds(pl.multiple_of(q * half, half), half), :],
            put_s.at[h],
        )

    def b_spot(j):
        return bv.at[j // 8, pl.ds(pl.multiple_of(j % 8 * depth, depth), depth), :]

    def b_in(j):
        return pltpu.make_async_copy(b.at[:, columns(q, j)], b_spot(j), put_s.at[8 + j])

    def b_out(j):
        return pltpu.make_async_copy(b_spot(j), b_rows(j, d), put_s.at[8 + j])

    @pl.loop(0, 8)
    def _(dev):
        own_in(dev).start()

    @pl.loop(0, tiles)
    def _(j):
        b_in(j).start()

    def b_copy(j, n):
        return remote(b.at[:, columns(peers[n], j)], b_rows(j, d), b_s, b_r.at[j, n], at(z, peers[n]))

    def b_landed(j, n):
        dst = b_rows(j, peers[n] * 2 + core)
        return remote(dst, dst, b_s, b_r.at[j, n], at(z, peers[n]))

    def b_own(j):
        return remote(b.at[:, columns(q, j)], b_rows(j, d), own_s, own_r.at[j], sibling)

    def b_pass(j, n):
        dst = b_rows(j, peers[n] * 2 + core)
        return remote(dst, dst, pass_s, pass_r.at[j, n], sibling)

    def b_passed(j, n):
        dst = b_rows(j, peers[n] * 2 + 1 - core)
        return remote(dst, dst, pass_s, pass_r.at[j, n], sibling)

    def b_own_passed(j):
        dst = b_rows(j, d + 1 - 2 * core)
        return remote(dst, dst, own_s, own_r.at[j], sibling)

    def a_x(g, chip):
        return remote(a_rows(g, chip), a_rows(g, chip), a_s, ax_r.at[g], at(z, q_x))

    def a_y(g, chip):
        return remote(a_rows(g, chip), a_rows(g, chip), a_s, ay_r.at[g], at(z, q_y))

    def f_y(g, chip):
        return remote(a_rows(g, chip, 0, quarter), a_rows(g, chip, 0, quarter), a_s, fy_r.at[g], at(z, q_y))

    def f_x(g, chip):
        return remote(a_rows(g, chip, quarter, quarter), a_rows(g, chip, quarter, quarter), a_s, fx_r.at[g], at(z, q_x))

    def up(g, j):
        return remote(part.at[g, j], low.at[g, j], up_s, low_r.at[g, j], at(jnp.minimum(z + 1, 3), q))

    def down(g, j):
        return remote(part.at[g, j], high.at[g, j], up_s, high_r.at[g, j], at(jnp.maximum(z - 1, 0), q))

    def send_part(g, j):
        @pl.when(g // 2 > z)
        def _():
            up(g, j).start()

        @pl.when(g // 2 < z)
        def _():
            down(g, j).start()

    def final(h, j, n):
        return remote(
            cv.at[h, j, pl.ds(pl.multiple_of(peers[n] * half, half), half), :],
            c_out.at[pl.ds(pl.multiple_of(h * half, half), half), columns(q, j)],
            fin_s, fin_r, at(z, peers[n]),
        )

    def final_own(h, j):
        return pltpu.make_async_copy(
            cv.at[h, j, pl.ds(pl.multiple_of(q * half, half), half), :],
            c_out.at[pl.ds(pl.multiple_of(h * half, half), half), columns(q, j)],
            fin_l,
        )

    def load_a(g, part_k, slot):
        span = pl.ds(part_k * 4 * depth, 4 * depth)
        return pltpu.make_async_copy(a_all.at[g, :, span], av.at[slot, :, span], lda.at[slot, part_k])

    def load_b(j, part_k, slot):
        span = pl.ds(part_k * 4 * depth, 4 * depth)
        return pltpu.make_async_copy(b_all.at[j, span, :], bv.at[slot, span, :], ldb.at[slot, part_k])

    def stored(g, j, slot, sent):
        pltpu.make_async_copy(acc.at[slot], part.at[g, j], st.at[slot]).wait()

        @pl.when(sent == 1)
        def _():
            send_part(g, j)

    def multiply(g, j, a_slot, b_slot, a_wait, b_wait, use, settle):
        for part_k in range(2):

            @pl.when(a_wait == 1)
            def _():
                load_a(g, part_k, a_slot).wait()

            @pl.when(b_wait == 1)
            def _():
                load_b(j, part_k, b_slot).wait()

            span = pl.ds(part_k * 4 * depth, 4 * depth)
            prod = jnp.dot(av[a_slot, :, span], bv[b_slot, span, :], preferred_element_type=jnp.float32)
            if part_k == 0:
                acc[use] = prod
                settle()
            else:
                acc[use] += prod

        pltpu.make_async_copy(acc.at[use], part.at[g, j], st.at[use]).start()

    def add_up(g, j, use, settle, same):
        i, h = g // 2, g % 2
        has_low = (z > 0) & (z <= i)
        has_high = (z < 3) & (z >= i)

        if True:
            mine = pltpu.make_async_copy(part.at[g, j], s0.at[use], ls.at[0])
            below = pltpu.make_async_copy(low.at[g, j], s1, ls.at[1])
            above = pltpu.make_async_copy(high.at[g, j], s2, ls.at[2])
            @pl.when(same)
            def _():
                settle()

            mine.start()

            @pl.when(jnp.logical_not(same))
            def _():
                settle()

            @pl.when(has_low)
            def _():
                up(g, j).wait_recv()
                below.start()

            @pl.when(has_high)
            def _():
                down(g, j).wait_recv()
                above.start()

            mine.wait()

            @pl.when(has_low)
            def _():
                below.wait()
                s0[use] += s1[...]

            @pl.when(has_high)
            def _():
                above.wait()
                s0[use] += s2[...]

            @pl.when(i == z)
            def _():
                cv[h, j] = s0[use].astype(cv.dtype)
                for n in range(3):
                    final(h, j, n).start()
                final_own(h, j).start()

            @pl.when(i != z)
            def _():
                pltpu.make_async_copy(s0.at[use], part.at[g, j], st.at[use]).start()

    def run_step(code):
        fields = []
        for bits in FIELDS:
            fields.append(code % (1 << bits))
            code = code // (1 << bits)
        op, g, j, a_slot, b_slot, a_wait, b_wait, use, pending, last_g, last_j, last_use, sent = fields
        plane = jnp.where(z >= 2, 3 - g, g)
        g = jnp.where(z >= 2, 6 - g // 2 * 2 + g % 2, g)
        last_g = jnp.where(z >= 2, 6 - last_g // 2 * 2 + last_g % 2, last_g)

        def settle():
            @pl.when(pending == 1)
            def _():
                stored(last_g, last_j, last_use, sent)

        @pl.when((op != MULT) & (op != SUM))
        def _():
            settle()

        @pl.when(op == B_SEND)
        @jax.named_scope("b_send")
        def _():
            for n in range(3):
                b_copy(j, n).start()
            b_own(j).start()

        @pl.when(op == B_PASS)
        @jax.named_scope("b_pass")
        def _():
            for n in range(3):
                b_landed(j, n).wait_recv()
                b_pass(j, n).start()

        @pl.when(op == B_HAVE)
        @jax.named_scope("b_have")
        def _():
            b_own_passed(j).wait_recv()
            for n in range(3):
                b_passed(j, n).wait_recv()

        @pl.when(op == A_SEND)
        @jax.named_scope("a_send")
        def _():
            @pl.when(g // 2 != z)
            def _():
                landed = a_rows(g, q)
                remote(landed, landed, a1_s, a1_r.at[g], at(z, q_x)).wait_recv()

            a_x(g, q).start()
            a_y(g, q).start()

        @pl.when(op == A_PASS)
        @jax.named_scope("a_pass")
        def _():
            a_x(g, q_x).wait_recv()
            f_y(g, q_x).start()
            a_y(g, q_y).wait_recv()
            f_x(g, q_y).start()

        @pl.when(op == A_HAVE)
        @jax.named_scope("a_have")
        def _():
            f_y(g, q_d).wait_recv()
            f_x(g, q_d).wait_recv()

        @pl.when(op == A_OUT)
        def _():
            @pl.loop(0, 8)
            def _(dev):
                a_out(plane, j, dev).start()

        @pl.when(op == LOAD_A)
        def _():
            for part_k in range(2):
                load_a(g, part_k, a_slot).start()

        @pl.when(op == LOAD_B)
        def _():
            for part_k in range(2):
                load_b(j, part_k, b_slot).start()

        @pl.when(op == PUT)
        def _():
            @pl.loop(0, 8)
            def _(dev):
                own_in(dev).wait()

            for h in range(2):
                own_out(h).start()

            @pl.loop(0, tiles)
            def _(n):
                b_in(n).wait()
                b_out(n).start()

        @pl.when(op == PUT_DONE)
        def _():
            for h in range(2):
                own_out(h).wait()

            @pl.loop(0, tiles)
            def _(n):
                b_out(n).wait()

        @pl.when(op == MULT)
        @jax.named_scope("mult")
        def _():
            multiply(g, j, a_slot, b_slot, a_wait, b_wait, use, settle)

        @pl.when(op == SUM)
        @jax.named_scope("sum")
        def _():
            add_up(g, j, use, settle, (last_g == g) & (last_j == j))

    def codes(steps):
        packed = []
        for step in steps:
            code, at_bit = 0, 0
            for value, bits in zip(step, FIELDS, strict=True):
                code |= value << at_bit
                at_bit += bits
            packed.append(code)
        return packed

    end_codes, mid_codes = codes(end_steps), codes(mid_steps)
    blocks = -(-max(len(end_codes), len(mid_codes)) // BLOCK)
    table = [c + [NOTHING] * (blocks * BLOCK - len(c)) for c in (end_codes, mid_codes)]
    is_mid = jnp.where((z == 1) | (z == 2), blocks, 0)

    @pl.loop(0, blocks)
    def _(block):
        now = [choose(block + is_mid, [jnp.int32(v) for c in table for v in c[n::BLOCK]]) for n in range(BLOCK)]

        @pl.loop(0, BLOCK)
        def _(n):
            run_step(choose(n, now))

    def all_done(like, sem):
        pltpu.make_async_copy(like, like, sem).wait()

    with jax.named_scope("drain"):
        for sem, count in ((b_s, 3), (pass_s, 3), (own_s, 1)):
            all_done(b.at[:, pl.ds(0, count * wide)], sem)
        all_done(a.at[:, pl.ds(0, 24 * depth)], a1_s)
        all_done(a_all.at[pl.ds(0, 6)], a_s)
        all_done(c_out.at[:, pl.ds(0, wide)], fin_l)
        all_done(part.at[pl.ds(0, 6)], up_s)
        for sem in (fin_s, fin_r):
            all_done(c_out.at[:, pl.ds(0, 3 * wide)], sem)


def solution(mesh):
    spec_rows = P(("dp", "tp"), None)

    def local_block(a, b):
        rows, depth, cols = a.shape[0], b.shape[0], b.shape[1]
        wide = cols // 4
        tile = min(TILE, wide // 9)
        tiles = wide // tile
        group = 2 * rows
        dma = pltpu.SemaphoreType.DMA
        any_space = pl.BlockSpec(memory_space=pl.ANY)
        out = pl.pallas_call(
            functools.partial(kernel, make_steps(END_ORDER, 0), make_steps(MID_ORDER, 1)),
            out_shape=[
                jax.ShapeDtypeStruct((rows, cols), jnp.bfloat16),
                jax.ShapeDtypeStruct((8, group, 8 * depth), jnp.bfloat16),
                jax.ShapeDtypeStruct((tiles, 8 * depth, tile), jnp.bfloat16),
                jax.ShapeDtypeStruct((8, tiles, group, tile), jnp.float32),
                jax.ShapeDtypeStruct((8, tiles, group, tile), jnp.float32),
                jax.ShapeDtypeStruct((8, tiles, group, tile), jnp.float32),
            ],
            in_specs=[any_space] * 2,
            out_specs=[any_space] * 6,
            scratch_shapes=[
                pltpu.VMEM((A_SLOTS, group, 8 * depth), jnp.bfloat16),
                pltpu.VMEM((B_SLOTS, 8 * depth, tile), jnp.bfloat16),
                pltpu.VMEM((2, group, tile), jnp.float32),
                pltpu.VMEM((2, group, tile), jnp.float32),
                pltpu.VMEM((group, tile), jnp.float32),
                pltpu.VMEM((group, tile), jnp.float32),
                pltpu.VMEM((2, tiles, group, tile), jnp.bfloat16),
                dma, dma((8,)), dma, dma((8,)), dma((8,)), dma((8,)), dma((8,)),
                dma, dma((tiles, 3)), dma, dma((tiles,)), dma, dma((tiles, 3)),
                dma, dma((8, tiles)), dma((8, tiles)), dma, dma, dma,
                dma((A_SLOTS, 2)), dma((B_SLOTS, 2)), dma((2,)), dma((3,)), dma((8 + tiles,)),
            ],
            compiler_params=pltpu.CompilerParams(
                collective_id=0, has_side_effects=True, vmem_limit_bytes=60 * 1024 * 1024
            ),
        )(a, b)
        return out[0]

    return jax.shard_map(local_block, mesh=mesh, in_specs=(spec_rows, spec_rows), out_specs=spec_rows, check_vma=False)
```

```python
import functools

import jax
import jax.numpy as jnp
from jax import lax
from jax.experimental import pallas as pl
from jax.experimental.pallas import tpu as pltpu
from jax.sharding import PartitionSpec as P

TILE = 384
B_SEND, B_PASS, B_HAVE, A_SEND, A_PASS, A_HAVE, MULT, SUM, A_OUT, LOAD_A, LOAD_B, PUT, PUT_DONE, NOTHING = range(14)

END_ORDER = (
    931100911930101200921450, 201470550570910301650751, 300750460670771920770102, 560202302752772103660762,
    761760440203303753763773, 540104640743742741740105, 204304744754764774106205, 305745755765775430206306,
    746756766776530410630736, 735734733732731730510107, 610716715714713712711710, 816815814813812207811810,
    307717737747108757767777, 420208308718738748758768, 778520400620728727726725, 724723722721500720817600,
    708707706705704703702701, 700808818807806805804803, 802801800,
)
MID_ORDER = (
    900901931100101920102200, 410201202921510470300610, 710930301711302712570450, 670770771871772550460400,
    870650750850751851752852, 810811872560812500103660, 760104860761861762862600, 700800701702801105802203,
    303753853763863773873106, 703713803204304754854813, 764864774440874704714205, 804305755855765814865775,
    875705715805206306756856, 815766866776706716540430, 876806816640740840741841, 742842743843744844530107,
    745108845746846630730731, 831732830832733833734834, 735835736207836420307747, 847757857767867777737877,
    707208837717308748758807, 848768817778858738708718, 868838520878808818620720, 721722723724725726825826,
    727827824728828823822821, 820,
)


FIELDS = (4, 3, 4, 2, 2, 1, 1, 1, 1, 3, 4, 1, 1)
A_SLOTS, B_SLOTS, BLOCK = 4, 3, 16


def make_steps(order, own):
    text = "".join(map(str, order))
    ops = [(int(text[n]) - 1, int(text[n + 1]), int(text[n + 2])) for n in range(0, len(text), 3)]
    have = {op: n for n, op in enumerate(ops)}
    before = [[] for _ in ops]
    held = {LOAD_A: [None] * A_SLOTS, LOAD_B: [None] * B_SLOTS}
    used = {LOAD_A: [-1] * A_SLOTS, LOAD_B: [-1] * B_SLOTS}
    last = -1
    mults = {}
    for n, (op, g, j) in enumerate(ops):
        if op != MULT:
            continue
        wait, slot = {}, {}
        for load, what, ready in ((LOAD_B, j, have[(B_HAVE, 0, j)]), (LOAD_A, g, have[(A_HAVE, g, 0)])):
            wait[load] = int(what not in held[load])
            if wait[load]:
                slot[load] = used[load].index(min(used[load]))
                held[load][slot[load]] = what
                before[max(last, ready + 1)].append((load, g, j, slot[load]))
            else:
                slot[load] = held[load].index(what)
            used[load][slot[load]] = n
        mults[n] = (slot[LOAD_A], slot[LOAD_B], wait[LOAD_A], wait[LOAD_B])
        last = n
    steps = []
    pending, store = (0, 0, 0, 0, 0), 0
    first = next(n for n, op in enumerate(ops) if op[0] in (B_PASS, B_HAVE, A_SEND))

    def step(op, g, j, a_slot=0, b_slot=0, a_wait=0, b_wait=0, use=0):
        nonlocal pending
        steps.append((op, g, j, a_slot, b_slot, a_wait, b_wait, use, *pending))
        pending = (0, 0, 0, 0, 0)

    for n, (op, g, j) in enumerate(ops):
        for load, lg, lj, ls in before[n]:
            step(load, lg, lj, ls, ls)
        if n == first:
            step(PUT, 0, 0)
        if n == first + 1:
            step(PUT_DONE, 0, 0)
        step(op, g, j, *mults.get(n, (0, 0, 0, 0)), store)
        if op == MULT or (op == SUM and g // 2 != own):
            pending = (1, g, j, store, int((op == MULT) == (own == 0) and g // 2 != own))
            store = 1 - store
    step(NOTHING, 0, 0)
    return steps


def padded(steps, count):
    at = next(n for n, s in enumerate(steps) if s[0] == PUT) + 1
    idle = (NOTHING,) + (0,) * (len(FIELDS) - 1)
    return steps[:at] + [idle] * (count - len(steps)) + steps[at:]


def choose(index, values):
    out = jnp.int32(values[-1])
    for k in range(len(values) - 2, -1, -1):
        out = jnp.where(index <= k, values[k], out)
    return out


def kernel(
    end_steps, mid_steps, a, b, c_out, a_all, b_all, part, low, high,
    av, bv, acc, s0, s1, s2, cv,
    a1_s, a1_r, a_s, ax_r, ay_r, f_r,
    b_s, b_r, own_s, pass_s, have_r, up_s, z_r, fin_s, fin_r, fin_l, lda, ldb, st, ls, put_s,
):
    rows, depth = a.shape[0], b.shape[0]
    tile = part.shape[3]
    tiles = part.shape[1]
    wide = tile * tiles
    half, quarter = rows // 2, rows // 4
    z, d = lax.axis_index("tp"), lax.axis_index("dp")
    q = d // 2
    core, x, y = d % 2, q % 2, d // 4
    q_x, q_y = q + 1 - 2 * x, q + 2 - 4 * y
    q_d = q_x + 2 - 4 * y
    peers = (q_x, q_y, q_d)

    def at(plane, chip):
        return {"tp": plane, "dp": chip * 2 + core}

    sibling = {"tp": z, "dp": d + 1 - 2 * core}

    def remote(src, dst, send, recv, to):
        return pltpu.make_async_remote_copy(
            src_ref=src, dst_ref=dst, send_sem=send, recv_sem=recv, device_id=to, device_id_type=pl.DeviceIdType.MESH
        )

    def a_rows(g, chip, first=0, count=half):
        return a_all.at[g, pl.ds(pl.multiple_of(chip * half + first, quarter), count), :]

    def b_rows(j, dev):
        return b_all.at[j, pl.ds(pl.multiple_of(dev * depth, depth), depth), :]

    def columns(chip, j):
        return pl.ds(pl.multiple_of(chip * wide + j * tile, tile), tile)

    def k_block(dev, plane):
        return pl.ds(pl.multiple_of((dev * 4 + plane) * depth, depth), depth)

    barrier = pltpu.get_barrier_semaphore()
    for plane in range(1, 4):
        pl.semaphore_signal(barrier, inc=1, device_id=at((z + plane) % 4, q), device_id_type=pl.DeviceIdType.MESH)
    for chip in peers:
        pl.semaphore_signal(barrier, inc=1, device_id=at(z, chip), device_id_type=pl.DeviceIdType.MESH)
    pl.semaphore_signal(barrier, inc=1, device_id=sibling, device_id_type=pl.DeviceIdType.MESH)
    pl.semaphore_wait(barrier, 7)

    def a_out(plane, h, dev):
        return remote(
            a.at[pl.ds(pl.multiple_of(h * half, half), half), k_block(dev, plane)],
            a_all.at[z * 2 + h, pl.ds(pl.multiple_of(q * half, half), half), pl.ds(pl.multiple_of(dev * depth, depth), depth)],
            a1_s, a1_r.at[z * 2 + h], at(plane, q),
        )

    def own_in(dev):
        return pltpu.make_async_copy(
            a.at[:, k_block(dev, z)], av.at[0, pl.ds(0, rows), pl.ds(pl.multiple_of(dev * depth, depth), depth)], put_s.at[0]
        )

    def own_out(h):
        return pltpu.make_async_copy(
            av.at[0, pl.ds(h * half, half), :],
            a_all.at[z * 2 + h, pl.ds(pl.multiple_of(q * half, half), half), :],
            put_s.at[0],
        )

    def b_spot(j):
        return bv.at[j // 8, pl.ds(pl.multiple_of(j % 8 * depth, depth), depth), :]

    def b_in(j):
        return pltpu.make_async_copy(b.at[:, columns(q, j)], b_spot(j), put_s.at[1 + j // 8])

    def b_out(j):
        return pltpu.make_async_copy(b_spot(j), b_rows(j, d), put_s.at[1 + j // 8])

    def put_wait():
        for like, n in ((av.at[0, pl.ds(0, rows), :], 0), (bv.at[0], 1), (bv.at[1, pl.ds(0, (tiles - 8) * depth), :], 2)):
            pltpu.make_async_copy(like, like, put_s.at[n]).wait()

    @pl.loop(0, 8)
    def _(dev):
        own_in(dev).start()

    @pl.loop(0, tiles)
    def _(j):
        b_in(j).start()

    def b_copy(j, n):
        return remote(b.at[:, columns(peers[n], j)], b_rows(j, d), b_s, b_r.at[j, n // 2], at(z, peers[n]))

    def b_landed(j, far):
        dst = b_all.at[j, pl.ds(0, depth if far else 2 * depth), :]
        return remote(dst, dst, b_s, b_r.at[j, far], at(z, peers[0]))

    def b_own(j):
        return remote(b.at[:, columns(q, j)], b_rows(j, d), own_s, have_r.at[j], sibling)

    def b_pass(j, n):
        dst = b_rows(j, peers[n] * 2 + core)
        return remote(dst, dst, pass_s, have_r.at[j], sibling)

    def b_passed(j):
        dst = b_all.at[j, pl.ds(0, 4 * depth), :]
        return remote(dst, dst, pass_s, have_r.at[j], sibling)

    def a_x(g, chip):
        return remote(a_rows(g, chip), a_rows(g, chip), a_s, ax_r.at[g], at(z, q_x))

    def a_y(g, chip):
        return remote(a_rows(g, chip), a_rows(g, chip), a_s, ay_r.at[g], at(z, q_y))

    def f_y(g, chip):
        return remote(a_rows(g, chip, 0, quarter), a_rows(g, chip, 0, quarter), a_s, f_r.at[g], at(z, q_y))

    def f_x(g, chip):
        return remote(a_rows(g, chip, quarter, quarter), a_rows(g, chip, quarter, quarter), a_s, f_r.at[g], at(z, q_x))

    def up(g, j):
        return remote(part.at[g, j], low.at[g, j], up_s, z_r.at[g, j], at(jnp.minimum(z + 1, 3), q))

    def own_or(g, receiver):
        return jnp.where(g // 2 == receiver, 8 + g % 2, g)

    def down(g, j, receiver):
        return remote(part.at[g, j], high.at[g, j], up_s, z_r.at[own_or(g, receiver), j], at(jnp.maximum(z - 1, 0), q))

    def send_part(g, j):
        @pl.when(g // 2 > z)
        def _():
            up(g, j).start()

        @pl.when(g // 2 < z)
        def _():
            down(g, j, z - 1).start()

    def final(h, j, n):
        return remote(
            cv.at[h, j, pl.ds(pl.multiple_of(peers[n] * half, half), half), :],
            c_out.at[pl.ds(pl.multiple_of(h * half, half), half), columns(q, j)],
            fin_s, fin_r, at(z, peers[n]),
        )

    def final_own(h, j):
        return pltpu.make_async_copy(
            cv.at[h, j, pl.ds(pl.multiple_of(q * half, half), half), :],
            c_out.at[pl.ds(pl.multiple_of(h * half, half), half), columns(q, j)],
            fin_l,
        )

    def load_a(g, part_k, slot):
        span = pl.ds(part_k * 4 * depth, 4 * depth)
        return pltpu.make_async_copy(a_all.at[g, :, span], av.at[slot, :, span], lda.at[slot, part_k])

    def load_b(j, part_k, slot):
        span = pl.ds(part_k * 4 * depth, 4 * depth)
        return pltpu.make_async_copy(b_all.at[j, span, :], bv.at[slot, span, :], ldb.at[slot, part_k])

    def stored(g, j, slot, sent):
        pltpu.make_async_copy(acc.at[slot], part.at[g, j], st.at[slot]).wait()

        @pl.when(sent == 1)
        def _():
            send_part(g, j)

    def multiply(g, j, a_slot, b_slot, a_wait, b_wait, use, settle):
        for part_k in range(2):

            @pl.when(a_wait == 1)
            def _():
                load_a(g, part_k, a_slot).wait()

            @pl.when(b_wait == 1)
            def _():
                load_b(j, part_k, b_slot).wait()

            span = pl.ds(part_k * 4 * depth, 4 * depth)
            prod = jnp.dot(av[a_slot, :, span], bv[b_slot, span, :], preferred_element_type=jnp.float32)
            if part_k == 0:
                acc[use] = prod
                settle()
            else:
                acc[use] += prod

        pltpu.make_async_copy(acc.at[use], part.at[g, j], st.at[use]).start()

    def add_up(g, j, use, settle, same):
        i, h = g // 2, g % 2
        has_low = (z > 0) & (z <= i)
        has_high = (z < 3) & (z >= i)

        if True:
            mine = pltpu.make_async_copy(part.at[g, j], s0.at[use], ls.at[0])
            below = pltpu.make_async_copy(low.at[g, j], s1, ls.at[1])
            above = pltpu.make_async_copy(high.at[g, j], s2, ls.at[2])
            @pl.when(same)
            def _():
                settle()

            mine.start()

            @pl.when(jnp.logical_not(same))
            def _():
                settle()

            @pl.when(has_low)
            def _():
                up(g, j).wait_recv()
                below.start()

            @pl.when(has_high)
            def _():
                down(g, j, z).wait_recv()
                above.start()

            mine.wait()

            @pl.when(has_low)
            def _():
                below.wait()
                s0[use] += s1[...]

            @pl.when(has_high)
            def _():
                above.wait()
                s0[use] += s2[...]

            @pl.when(i == z)
            def _():
                cv[h, j] = s0[use].astype(cv.dtype)
                for n in range(3):
                    final(h, j, n).start()
                final_own(h, j).start()

            @pl.when(i != z)
            def _():
                pltpu.make_async_copy(s0.at[use], part.at[g, j], st.at[use]).start()

    def run_step(code):
        fields = []
        for bits in FIELDS:
            fields.append(lax.rem(code, jnp.int32(1 << bits)))
            code = lax.div(code, jnp.int32(1 << bits))
        op, g, j, a_slot, b_slot, a_wait, b_wait, use, pending, last_g, last_j, last_use, sent = fields
        plane = jnp.where(z >= 2, 3 - g, g)
        g = jnp.where(z >= 2, 6 - g // 2 * 2 + g % 2, g)
        last_g = jnp.where(z >= 2, 6 - last_g // 2 * 2 + last_g % 2, last_g)

        def settle():
            @pl.when(pending == 1)
            def _():
                stored(last_g, last_j, last_use, sent)

        @pl.when((op != MULT) & (op != SUM))
        def _():
            settle()

        @pl.when(op == B_SEND)
        @jax.named_scope("b_send")
        def _():
            for n in range(3):
                b_copy(j, n).start()
            b_own(j).start()

        @pl.when(op == B_PASS)
        @jax.named_scope("b_pass")
        def _():
            for far in range(2):
                b_landed(j, far).wait_recv()
                for n in range(2 * far, 2 + far):
                    b_pass(j, n).start()

        @pl.when(op == B_HAVE)
        @jax.named_scope("b_have")
        def _():
            b_passed(j).wait_recv()

        @pl.when(op == A_SEND)
        @jax.named_scope("a_send")
        def _():
            @pl.when(g // 2 != z)
            def _():
                landed = a_rows(g, q)
                remote(landed, landed, a1_s, a1_r.at[g], at(z, q_x)).wait_recv()

            a_x(g, q).start()
            a_y(g, q).start()

        @pl.when(op == A_PASS)
        @jax.named_scope("a_pass")
        def _():
            a_x(g, q_x).wait_recv()
            f_y(g, q_x).start()
            a_y(g, q_y).wait_recv()
            f_x(g, q_y).start()

        @pl.when(op == A_HAVE)
        @jax.named_scope("a_have")
        def _():
            remote(a_rows(g, q_d), a_rows(g, q_d), a_s, f_r.at[g], at(z, q_x)).wait_recv()

        @pl.when(op == A_OUT)
        def _():
            @pl.loop(0, 8)
            def _(dev):
                a_out(plane, j, dev).start()

        @pl.when(op == LOAD_A)
        def _():
            for part_k in range(2):
                load_a(g, part_k, a_slot).start()

        @pl.when(op == LOAD_B)
        def _():
            for part_k in range(2):
                load_b(j, part_k, b_slot).start()

        @pl.when(op == PUT)
        def _():
            put_wait()
            for h in range(2):
                own_out(h).start()

            @pl.loop(0, tiles)
            def _(n):
                b_out(n).start()

        @pl.when(op == PUT_DONE)
        def _():
            put_wait()

        @pl.when(op == MULT)
        @jax.named_scope("mult")
        def _():
            multiply(g, j, a_slot, b_slot, a_wait, b_wait, use, settle)

        @pl.when(op == SUM)
        @jax.named_scope("sum")
        def _():
            add_up(g, j, use, settle, (last_g == g) & (last_j == j))

    def codes(steps):
        packed = []
        for step in steps:
            code, at_bit = 0, 0
            for value, bits in zip(step, FIELDS, strict=True):
                code |= value << at_bit
                at_bit += bits
            packed.append(code)
        return packed

    blocks = -(-max(len(end_steps), len(mid_steps)) // BLOCK)
    table = [codes(padded(steps, blocks * BLOCK)) for steps in (end_steps, mid_steps)]
    is_mid = jnp.where((z == 1) | (z == 2), blocks, 0)

    @pl.loop(0, blocks)
    def _(block):
        now = [choose(block + is_mid, [jnp.int32(v) for c in table for v in c[n::BLOCK]]) for n in range(BLOCK)]

        @pl.loop(0, BLOCK)
        def _(n):
            run_step(choose(n, now))

    def all_done(like, sem):
        pltpu.make_async_copy(like, like, sem).wait()

    with jax.named_scope("drain"):
        for sem, count in ((b_s, 3), (pass_s, 3), (own_s, 1)):
            all_done(b.at[:, pl.ds(0, count * wide)], sem)
        all_done(a.at[:, pl.ds(0, 24 * depth)], a1_s)
        all_done(a_all.at[pl.ds(0, 6)], a_s)
        all_done(c_out.at[:, pl.ds(0, wide)], fin_l)
        all_done(part.at[pl.ds(0, 6)], up_s)
        for sem in (fin_s, fin_r):
            all_done(c_out.at[:, pl.ds(0, 3 * wide)], sem)


def solution(mesh):
    spec_rows = P(("dp", "tp"), None)

    def local_block(a, b):
        rows, depth, cols = a.shape[0], b.shape[0], b.shape[1]
        wide = cols // 4
        tile = min(TILE, wide // 9)
        tiles = wide // tile
        group = 2 * rows
        dma = pltpu.SemaphoreType.DMA
        any_space = pl.BlockSpec(memory_space=pl.ANY)
        out = pl.pallas_call(
            functools.partial(kernel, make_steps(END_ORDER, 0), make_steps(MID_ORDER, 1)),
            out_shape=[
                jax.ShapeDtypeStruct((rows, cols), jnp.bfloat16),
                jax.ShapeDtypeStruct((8, group, 8 * depth), jnp.bfloat16),
                jax.ShapeDtypeStruct((tiles, 8 * depth, tile), jnp.bfloat16),
                jax.ShapeDtypeStruct((8, tiles, group, tile), jnp.float32),
                jax.ShapeDtypeStruct((8, tiles, group, tile), jnp.float32),
                jax.ShapeDtypeStruct((8, tiles, group, tile), jnp.float32),
            ],
            in_specs=[any_space] * 2,
            out_specs=[any_space] * 6,
            scratch_shapes=[
                pltpu.VMEM((A_SLOTS, group, 8 * depth), jnp.bfloat16),
                pltpu.VMEM((B_SLOTS, 8 * depth, tile), jnp.bfloat16),
                pltpu.VMEM((2, group, tile), jnp.float32),
                pltpu.VMEM((2, group, tile), jnp.float32),
                pltpu.VMEM((group, tile), jnp.float32),
                pltpu.VMEM((group, tile), jnp.float32),
                pltpu.VMEM((2, tiles, group, tile), jnp.bfloat16),
                dma, dma((8,)), dma, dma((8,)), dma((8,)), dma((8,)),
                dma, dma((tiles, 2)), dma, dma, dma((tiles,)), dma, dma((10, tiles)), dma, dma, dma,
                dma((A_SLOTS, 2)), dma((B_SLOTS, 2)), dma((2,)), dma((3,)), dma((3,)),
            ],
            compiler_params=pltpu.CompilerParams(
                collective_id=0, has_side_effects=True, vmem_limit_bytes=60 * 1024 * 1024
            ),
        )(a, b)
        return out[0]

    return jax.shard_map(local_block, mesh=mesh, in_specs=(spec_rows, spec_rows), out_specs=spec_rows, check_vma=False)
```
